256 devices in a mesh: row: 16 (over y_hi, x, core), col: 16 (over z, y_lo).
Axes of the slice: x: 4, y: 4 (y_hi: 2, y_lo: 2; y = y_hi * 2 + y_lo), z: 8, core: 2. Of those that a mesh axis runs over, the one named last changes fastest.
Arguments:
- rho_real: float32 [8192, 8192], P('row', 'col'), may hold values from -6 to 12, as said below
- rho_imag: float32 [8192, 8192], P('row', 'col'), may hold values from -6 to 6, as said below
- gate_real_matrix: float32 [16, 16], replicated, may hold values from -1 to 1, as said below
- gate_imaginary: float32 [16, 16], replicated, may hold values from -1 to 1, as said below
- angles: float32 [8, 3], replicated, may hold values from -3.140625 to 3.140625
- targets: int32 [8], replicated, may hold values from 0 to 4
- gate_order: int32 [8], replicated, may hold values from 0 to 7, each once
Outputs:
- mixed_real: float32 [8192, 8192], P('row', 'col')
- depolarized_quadrature: float32 [8192, 8192], P('row', 'col')
- purity: float32 [], replicated
The draws below stay inside these ranges and needn't reach their ends.
Inputs may be any that keep to these rules, and one draw needn't show every extreme that they name: rho_real is symmetric: entries of order one off the diagonal, each diagonal entry raised by 2 to 6. rho_imag is antisymmetric with a zero diagonal, so that rho_real + i rho_imag is Hermitian. gate_real_matrix + i gate_imaginary is a unitary matrix. gate_real_matrix + i gate_imaginary is a unitary matrix. `targets`: each gate acts on one of the 5 low qubits. `gate_order`: each gate appears once.
All inputs are finite; a program needn't handle non-finite values.
Results may differ from the reference program's by a relative error of at most 0.0001.
Values sent between devices are 32-bit elements; how exact they have to be, the bound alone decides.
No kernel may reach another device: no remote copies, remote signals or barrier semaphores. Data moves between devices by JAX's collectives and lax.ppermute only.
A program may use at most 64 MiB of HBM per device.

```python
import jax
import jax.numpy as jnp
from jax import lax

LQ = 5
GATE = 16
GATES = 8
DIM = 8192


def mirrored_weights(key):
    return jnp.ones((DIM,), jnp.float32)


def raw_noise(key):
    return jnp.clip(jax.random.normal(key, (DIM, DIM), jnp.float32), -6.0, 6.0)


def draw_rho_real(key, part):
    noise_key = jax.random.fold_in(key, 11)
    scale_key = jax.random.fold_in(key, 12)
    raise_key = jax.random.fold_in(key, 13)
    values = raw_noise(noise_key)
    values = 0.5 * (values + values.T)
    scales = mirrored_weights(scale_key)
    values = values * scales[:, None] * scales[None, :]
    raises = jax.random.uniform(raise_key, (DIM,), jnp.float32, 2.0, 6.0)
    on_diag = lax.broadcasted_iota(jnp.int32, (DIM, DIM), 0) == lax.broadcasted_iota(jnp.int32, (DIM, DIM), 1)
    return values + jnp.where(on_diag, raises[None, :], jnp.zeros_like(values))


def draw_rho_imag(key, part):
    noise_key = jax.random.fold_in(key, 21)
    scale_key = jax.random.fold_in(key, 22)
    values = raw_noise(noise_key)
    values = 0.5 * (values - values.T)
    scales = mirrored_weights(scale_key)
    return values * scales[:, None] * scales[None, :]


def unitary_parts(key):
    shared = jax.random.fold_in(key, 31)
    real_key = jax.random.fold_in(shared, 1)
    imag_key = jax.random.fold_in(shared, 2)
    first = jax.random.normal(real_key, (GATE, GATE), jnp.float32)
    second = jax.random.normal(imag_key, (GATE, GATE), jnp.float32)
    whole = lax.complex(first, second)
    factor_q, factor_r = jnp.linalg.qr(whole)
    diag_r = jnp.diagonal(factor_r)
    phases = diag_r / jnp.maximum(jnp.abs(diag_r), 0.001)
    unitary = factor_q * phases[None, :]
    return (jnp.real(unitary).astype(jnp.float32), jnp.imag(unitary).astype(jnp.float32))


def draw_gate_real_matrix(key, part):
    return unitary_parts(key)[0]


def draw_gate_imaginary(key, part):
    return unitary_parts(key)[1]


def place_ends(array, stream_key, low, largest):
    shape = array.shape
    spot = [jax.random.randint(jax.random.fold_in(stream_key, axis), (), 0, shape[axis]) for axis in range(len(shape))]
    array = array.at[tuple(spot)].set(low)
    longest = shape.index(max(shape))
    spot[longest] = (spot[longest] + 1) % shape[longest]
    return array.at[tuple(spot)].set(largest)


def setup_inputs(seed: int = 0) -> dict:
    splits = jax.random.split(jax.random.key(seed), 8)
    rho_real = draw_rho_real(jax.random.fold_in(splits[7], 71), 0)
    rho_imag = draw_rho_imag(jax.random.fold_in(splits[7], 71), 0)
    gate_real_matrix = draw_gate_real_matrix(jax.random.fold_in(splits[7], 71), 0)
    gate_imaginary = draw_gate_imaginary(jax.random.fold_in(splits[7], 71), 0)
    angles = jnp.clip(jax.random.uniform(splits[4], (GATES, 3), jnp.float32, -3.140625, 3.140625), -3.140625, 3.140625)
    targets = place_ends(jax.random.randint(splits[5], (GATES,), 0, LQ), jax.random.fold_in(splits[5], 1), 0, LQ - 1).astype(jnp.int32)
    gate_order = jax.random.permutation(splits[6], GATES).astype(jnp.int32)
    return dict(rho_real=rho_real, rho_imag=rho_imag, gate_real_matrix=gate_real_matrix, gate_imaginary=gate_imaginary, angles=angles, targets=targets, gate_order=gate_order)


highest = lax.Precision.HIGHEST
mixing = 0.25

def complex_blend(pattern, left_real, left_imag, right_real, right_imag):
    real_part = jnp.einsum(pattern, left_real, right_real, precision=highest) - jnp.einsum(pattern, left_imag, right_imag, precision=highest)
    imag_part = jnp.einsum(pattern, left_real, right_imag, precision=highest) + jnp.einsum(pattern, left_imag, right_real, precision=highest)
    return (real_part, imag_part)

def embed_gate(angle_row, target, low_width):
    half_turn = angle_row[0] / 2
    cosine_half = jnp.cos(half_turn)
    sine_half = jnp.sin(half_turn)
    phase_first = angle_row[1]
    phase_second = angle_row[2]
    element_count = ((cosine_half, cosine_half * 0.0), (-jnp.cos(phase_second) * sine_half, -jnp.sin(phase_second) * sine_half), (jnp.cos(phase_first) * sine_half, jnp.sin(phase_first) * sine_half), (jnp.cos(phase_first + phase_second) * cosine_half, jnp.sin(phase_first + phase_second) * cosine_half))
    left_index = lax.broadcasted_iota(jnp.int32, (low_width, low_width), 0)
    right_index = lax.broadcasted_iota(jnp.int32, (low_width, low_width), 1)
    target_bit = jnp.left_shift(jnp.ones((), jnp.int32), target.astype(jnp.int32))
    same_rest = jnp.bitwise_or(jnp.bitwise_xor(left_index, right_index), target_bit) == target_bit
    left_high = jnp.bitwise_and(left_index, target_bit) > 0
    right_high = jnp.bitwise_and(right_index, target_bit) > 0
    result = []
    for member in range(2):
        chosen = jnp.where(left_high, jnp.where(right_high, element_count[3][member], element_count[2][member]), jnp.where(right_high, element_count[1][member], element_count[0][member]))
        result.append(jnp.where(same_rest, chosen, jnp.zeros_like(chosen)))
    return (result[0], result[1])

def joined_gate(angles, targets, gate_order, low_width):
    gate_count = angles.shape[0]
    slot_ids = jnp.arange(gate_count, dtype=jnp.int32)
    total_real = jnp.eye(low_width, dtype=jnp.float32)
    total_imag = jnp.zeros((low_width, low_width), jnp.float32)
    for position in range(gate_count):
        picked = slot_ids == gate_order[position].astype(jnp.int32)
        angle_row = jnp.sum(jnp.where(picked[:, None], angles, jnp.zeros_like(angles)), axis=0)
        target = jnp.sum(jnp.where(picked, targets, jnp.zeros_like(targets))).astype(jnp.int32)
        step_real, step_imag = embed_gate(angle_row, target, low_width)
        total_real, total_imag = complex_blend('ab,bc->ac', step_real, step_imag, total_real, total_imag)
    return (total_real, total_imag)

def reference(rho_real, rho_imag, gate_real_matrix, gate_imaginary, angles, targets, gate_order):
    low_width = 2 ** LQ
    block_inphase_component, block_quadrature = joined_gate(angles, targets, gate_order, low_width)

    def row_block(segment_list):
        center_divide = complex_blend('xi,ifo->xfo', gate_real_matrix, gate_imaginary, segment_list[0], segment_list[1])
        return complex_blend('hf,ofg->ohg', block_inphase_component, block_quadrature, center_divide[0], center_divide[1])
    split_real = jnp.transpose(rho_real.reshape(GATE, GATE, low_width, DIM), (1, 0, 2, 3))
    split_imag = jnp.transpose(rho_imag.reshape(GATE, GATE, low_width, DIM), (1, 0, 2, 3))
    rows_real, rows_imag = lax.map(row_block, (split_real, split_imag))

    def col_block(segment_list):
        center_divide = complex_blend('rghl,Gg->rhGl', segment_list[0], segment_list[1], gate_real_matrix, -gate_imaginary)
        return complex_blend('rhGl,Ll->rhGL', center_divide[0], center_divide[1], block_inphase_component, -block_quadrature)
    block_rows = 512
    block_count = DIM // block_rows
    col_real, col_imag = lax.map(col_block, (rows_real.reshape(block_count, block_rows, GATE, GATE, low_width), rows_imag.reshape(block_count, block_rows, GATE, GATE, low_width)))
    col_real = col_real.reshape(DIM, DIM)
    col_imag = col_imag.reshape(DIM, DIM)
    trace_real = jnp.trace(col_real)
    trace_imag = jnp.trace(col_imag)
    diag_index = jnp.arange(DIM, dtype=jnp.int32)
    mixed_real = ((1 - mixing) * col_real).at[diag_index, diag_index].add(mixing * trace_real / DIM)
    depolarized_quadrature = ((1 - mixing) * col_imag).at[diag_index, diag_index].add(mixing * trace_imag / DIM)
    purity = (jnp.sum(mixed_real * mixed_real) + jnp.sum(depolarized_quadrature * depolarized_quadrature)) / (DIM * DIM)
    return (mixed_real, depolarized_quadrature, purity)
```

```python
import functools

import jax
import jax.numpy as jnp
from jax import lax
from jax.experimental import pallas as pl
from jax.experimental.pallas import tpu as pltpu
from jax.sharding import PartitionSpec as P

LQ = 5
LOW = 2**LQ
GATE = 16
GATES = 8
DIM = 8192
ROW_COL = ("row", "col")

MIXING = 0.25
KEEP = 1 - MIXING

LANES = 128
SUB = 8
QUADS = LANES // LOW
BLOCK = GATE * LOW
PAIRS = GATE * GATE
DATA_ROWS = 2 * LOW * LOW // LANES
SLOT = DATA_ROWS + 1
highest = lax.Precision.HIGHEST
f32 = jnp.float32
bf16 = jnp.bfloat16
VMEM = pl.BlockSpec(memory_space=pltpu.VMEM)
SMEM = pl.BlockSpec(memory_space=pltpu.SMEM)
ANY = pl.BlockSpec(memory_space=pl.ANY)
VMEM_LIMIT = 40 * 1024 * 1024


def iota(shape, dim):
    return lax.broadcasted_iota(jnp.int32, shape, dim)


def swap_quads(parts):
    lane = iota((SUB, LANES), 1)
    low_half = lane < LANES // 2
    even = jnp.bitwise_and(lane, LOW) == 0
    half = [None] * QUADS
    for a in (0, 1):
        first, second = parts[a], parts[a + 2]
        moving = pltpu.roll(jnp.where(low_half, second, first), LANES // 2, 1)
        half[a] = jnp.where(low_half, first, moving)
        half[a + 2] = jnp.where(low_half, moving, second)
    out = [None] * QUADS
    for a in (0, 2):
        first, second = half[a], half[a + 1]
        out[a] = jnp.where(even, first, pltpu.roll(second, LOW, 1))
        out[a + 1] = jnp.where(even, pltpu.roll(first, LANES - LOW, 1), second)
    return out


def split(value):
    high = value.astype(bf16)
    return high, (value - high.astype(f32)).astype(bf16)


def dot(left, right):
    return jnp.dot(left, right, preferred_element_type=f32)


def pack_kernel(flag_ref, real_hbm, imag_hbm, out_ref, real, imag, sems):
    chunks = 4
    rows = BLOCK // chunks
    copies = []
    for c in range(chunks):
        at = pl.ds(c * rows, rows)
        pair = (
            pltpu.make_async_copy(real_hbm.at[at], real.at[at], sems.at[0, c]),
            pltpu.make_async_copy(imag_hbm.at[at], imag.at[at], sems.at[1, c]),
        )
        for copy in pair:
            copy.start()
        copies.append(pair)
    squares = jnp.zeros((SUB, LANES), f32)
    diagonal = [jnp.zeros((SUB, LANES), f32), jnp.zeros((SUB, LANES), f32)]
    eye = iota((rows, LANES), 0) == iota((rows, LANES), 1)
    for c in range(chunks):
        for copy in copies[c]:
            copy.wait()

        def per_block(k, squares, c=c):
            h = c * (rows // LOW) + k
            for t in range(BLOCK // LANES):
                for part, ref in enumerate((real, imag)):
                    quads = [
                        ref[pl.ds(pl.multiple_of(h * LOW + p * SUB, SUB), SUB), t * LANES : (t + 1) * LANES]
                        for p in range(QUADS)
                    ]
                    for value in quads:
                        squares = squares + value * value
                    for q, value in enumerate(swap_quads(quads)):
                        slot = (h * GATE + t * QUADS + q) * SLOT
                        out_ref[pl.ds(slot + part, SUB, stride=2), :] = value
            return squares

        squares = lax.fori_loop(0, rows // LOW, per_block, squares)
        for part, ref in enumerate((real, imag)):
            square = ref[c * rows : (c + 1) * rows, c * LANES : (c + 1) * LANES]
            kept = jnp.where(eye, square, jnp.zeros_like(square))
            diagonal[part] = diagonal[part] + jnp.sum(kept.reshape(rows // SUB, SUB, LANES), axis=0)
    on_diagonal = flag_ref[0]
    trace_real = jnp.sum(diagonal[0])
    trace_imag = jnp.sum(diagonal[1])
    trace_real = jnp.where(on_diagonal == 1, trace_real, 0.0)
    trace_imag = jnp.where(on_diagonal == 1, trace_imag, 0.0)
    lane = iota((PAIRS, LANES), 1)
    sums = jnp.where(
        lane == 0, trace_real, jnp.where(lane == 1, trace_imag, jnp.where(lane == 2, jnp.sum(squares), 0.0))
    )
    out_ref[pl.ds(DATA_ROWS, PAIRS, stride=SLOT), :] = sums


def pack(flag, rho_real, rho_imag):
    return pl.pallas_call(
        pack_kernel,
        out_shape=jax.ShapeDtypeStruct((PAIRS * SLOT, LANES), f32),
        in_specs=[SMEM, ANY, ANY],
        out_specs=VMEM,
        scratch_shapes=[
            pltpu.VMEM((BLOCK, BLOCK), f32),
            pltpu.VMEM((BLOCK, BLOCK), f32),
            pltpu.SemaphoreType.DMA((2, 4)),
        ],
        compiler_params=pltpu.CompilerParams(vmem_limit_bytes=VMEM_LIMIT),
        name="pack",
    )(flag, rho_real, rho_imag)


def flip_rows(value, target):
    row = iota((LOW, LANES), 0)
    out = value
    for bit in range(LQ):
        step = 1 << bit
        up = pltpu.roll(value, LOW - step, 0)
        down = pltpu.roll(value, step, 0)
        flipped = jnp.where(jnp.bitwise_and(row, step) == 0, up, down)
        out = jnp.where(target == bit, flipped, out)
    return out


def gates_kernel(
    angles_ref, targets_ref, order_ref, ur_ref, ui_ref,
    right_hi, right_lo, left_hi, left_lo, top_hi, top_lo,
):
    row = iota((LOW, LANES), 0)
    lane = iota((LOW, LANES), 1)
    real = jnp.where(row == lane, 1.0, 0.0).astype(f32)
    imag = jnp.zeros((LOW, LANES), f32)
    slot = iota((SUB, LANES), 0)
    half = jnp.zeros((SUB, LANES), f32)
    first = jnp.zeros((SUB, LANES), f32)
    second = jnp.zeros((SUB, LANES), f32)
    for k in range(GATES):
        gate = order_ref[k]
        half = jnp.where(slot == k, angles_ref[gate, 0], half)
        first = jnp.where(slot == k, angles_ref[gate, 1], first)
        second = jnp.where(slot == k, angles_ref[gate, 2], second)
    half = half / 2
    both = first + second
    c, s = jnp.cos(half), jnp.sin(half)
    entries = (
        (c, jnp.zeros_like(c)),
        (-jnp.cos(second) * s, -jnp.sin(second) * s),
        (jnp.cos(first) * s, jnp.sin(first) * s),
        (jnp.cos(both) * c, jnp.sin(both) * c),
    )
    for k in range(GATES):
        target = targets_ref[order_ref[k]]
        high = jnp.bitwise_and(jnp.right_shift(row, target), 1) == 1
        low_low, low_high, high_low, high_high = (
            tuple(jnp.broadcast_to(member[k : k + 1, :], (LOW, LANES)) for member in entry)
            for entry in entries
        )
        same = [jnp.where(high, high_high[m], low_low[m]) for m in range(2)]
        other = [jnp.where(high, high_low[m], low_high[m]) for m in range(2)]
        flip_real = flip_rows(real, target)
        flip_imag = flip_rows(imag, target)
        real, imag = (
            same[0] * real - same[1] * imag + other[0] * flip_real - other[1] * flip_imag,
            same[0] * imag + same[1] * real + other[0] * flip_imag + other[1] * flip_real,
        )
    spread = jnp.where(iota((LOW, LANES), 0) == jnp.bitwise_and(lane, LOW - 1), 1.0, 0.0).astype(f32)
    wide = jnp.where(iota((LANES, LANES), 0) == jnp.bitwise_and(iota((LANES, LANES), 1), LOW - 1), 1.0, 0.0)
    group = jnp.right_shift(iota((LANES, LANES), 0), LQ) == jnp.right_shift(iota((LANES, LANES), 1), LQ)

    def blocks(value):
        across = jnp.dot(value, wide.astype(f32), precision=highest, preferred_element_type=f32)
        contract = functools.partial(
            lax.dot_general,
            dimension_numbers=(((0,), (0,)), ((), ())),
            precision=highest,
            preferred_element_type=f32,
        )
        plain = contract(spread, across)
        turned = contract(across, spread)
        return jnp.where(group, plain, 0.0), jnp.where(group, turned, 0.0)

    left_real, right_real = blocks(real)
    left_imag, right_imag = blocks(imag)

    def place(high_ref, low_ref, at_row, at_col, value):
        high, low = split(value)
        rows, cols = value.shape
        high_ref[at_row : at_row + rows, at_col : at_col + cols] = high
        low_ref[at_row : at_row + rows, at_col : at_col + cols] = low

    place(right_hi, right_lo, 0, 0, right_real)
    place(right_hi, right_lo, 0, LANES, -right_imag)
    place(right_hi, right_lo, LANES, 0, right_imag)
    place(right_hi, right_lo, LANES, LANES, right_real)
    place(left_hi, left_lo, 0, 0, KEEP * left_real)
    place(left_hi, left_lo, 0, LANES, -KEEP * left_imag)
    place(left_hi, left_lo, LANES, 0, KEEP * left_imag)
    place(left_hi, left_lo, LANES, LANES, KEEP * left_real)

    pair = iota((PAIRS, GATE), 0)
    gate = iota((PAIRS, GATE), 1)
    outer = jnp.where(jnp.right_shift(pair, 4) == gate, 1.0, 0.0).astype(f32)
    inner = jnp.where(jnp.bitwise_and(pair, GATE - 1) == gate, 1.0, 0.0).astype(f32)

    def expand(pick, value):
        rows = jnp.dot(pick, value, precision=highest, preferred_element_type=f32)
        return lax.dot_general(
            rows, pick, (((1,), (1,)), ((), ())), precision=highest, preferred_element_type=f32
        )

    outer_real, outer_imag = expand(outer, ur_ref[...]), expand(outer, ui_ref[...])
    inner_real, inner_imag = expand(inner, ur_ref[...]), expand(inner, ui_ref[...])
    top_real = outer_real * inner_real + outer_imag * inner_imag
    top_imag = outer_imag * inner_real - outer_real * inner_imag
    place(top_hi, top_lo, 0, 0, top_real)
    place(top_hi, top_lo, 0, PAIRS, -top_imag)
    place(top_hi, top_lo, PAIRS, 0, top_imag)
    place(top_hi, top_lo, PAIRS, PAIRS, top_real)


def gates(angles, targets, gate_order, gate_real, gate_imag):
    shapes = [(2 * LANES, 2 * LANES)] * 4 + [(2 * PAIRS, 2 * PAIRS)] * 2
    return pl.pallas_call(
        gates_kernel,
        out_shape=[jax.ShapeDtypeStruct(s, bf16) for s in shapes],
        in_specs=[SMEM, SMEM, SMEM, VMEM, VMEM],
        out_specs=[VMEM] * 6,
        compiler_params=pltpu.CompilerParams(vmem_limit_bytes=VMEM_LIMIT),
        cost_estimate=pl.CostEstimate(flops=2_000_000_000, bytes_accessed=1_600_000, transcendentals=8192),
        name="gates",
    )(angles, targets, gate_order, gate_real, gate_imag)


def apply_kernel(
    flag_ref, got, right_hi, right_lo, left_hi, left_lo, top_hi, top_lo,
    real_hbm, imag_hbm, purity_ref, turned, real, imag, sems,
):
    sums = jnp.sum(got[pl.ds(DATA_ROWS, PAIRS, stride=SLOT), :], axis=0, keepdims=True)
    lane = iota((1, LANES), 1)
    trace_real, trace_imag, squares = (jnp.sum(jnp.where(lane == k, sums, 0.0)) for k in range(3))
    purity_ref[0, 0] = (
        KEEP * KEEP * squares
        + (2 * KEEP * MIXING + MIXING * MIXING) * (trace_real * trace_real + trace_imag * trace_imag) / DIM
    ) / (DIM * DIM)
    shifts = [
        jnp.where(flag_ref[0] == 1, MIXING * trace / DIM, 0.0) for trace in (trace_real, trace_imag)
    ]

    for first in range(0, SUB, 2):
        halves = ([], [])
        for i in (first, first + 1):
            value = jnp.concatenate(
                [got[pl.ds(2 * i + part, PAIRS, stride=SLOT), :] for part in range(2)], axis=1
            )
            high, low = split(value)
            value = dot(high, right_hi[...]) + dot(low, right_hi[...]) + dot(high, right_lo[...])
            halves[0].append(value[:, :LANES])
            halves[1].append(value[:, LANES:])
        value = jnp.concatenate([jnp.concatenate(h, axis=1) for h in halves], axis=0)
        high, low = split(value)
        value = dot(top_hi[...], high) + dot(top_lo[...], high) + dot(top_hi[...], low)
        for j in range(2):
            for part in range(2):
                turned[pl.ds(2 * (first + j) + part, PAIRS, stride=SLOT), :] = value[
                    part * PAIRS : (part + 1) * PAIRS, j * LANES : (j + 1) * LANES
                ]

    rows = QUADS * LOW
    eye = iota((rows, LANES), 0) == iota((rows, LANES), 1)
    copies = []
    for block in range(GATE // QUADS):
        columns = []
        for t in range(GATE // QUADS):
            pieces = []
            for part in range(2):
                for g in range(QUADS):
                    quads = [
                        turned[pl.ds(((block * QUADS + g) * GATE + t * QUADS + q) * SLOT + part, SUB, stride=2), :]
                        for q in range(QUADS)
                    ]
                    pieces += swap_quads(quads)
            columns.append(jnp.concatenate(pieces, axis=0))
        value = jnp.concatenate(columns, axis=1)
        high, low = split(value)
        value = dot(left_hi[...], high) + dot(left_lo[...], high) + dot(left_hi[...], low)
        at = pl.ds(block * rows, rows)
        for part, ref in enumerate((real, imag)):
            ref[at, :] = value[part * rows : (part + 1) * rows, :]
            square = value[part * rows : (part + 1) * rows, block * LANES : (block + 1) * LANES]
            ref[at, block * LANES : (block + 1) * LANES] = square + jnp.where(eye, shifts[part], 0.0)
            copy = pltpu.make_async_copy(
                ref.at[at], (real_hbm, imag_hbm)[part].at[at], sems.at[part, block]
            )
            copy.start()
            copies.append(copy)
    for copy in copies:
        copy.wait()


def apply(flag, got, matrices):
    return pl.pallas_call(
        apply_kernel,
        out_shape=[
            jax.ShapeDtypeStruct((BLOCK, BLOCK), f32),
            jax.ShapeDtypeStruct((BLOCK, BLOCK), f32),
            jax.ShapeDtypeStruct((1, 1), f32),
        ],
        in_specs=[SMEM] + [VMEM] * 7,
        out_specs=[ANY, ANY, SMEM],
        scratch_shapes=[
            pltpu.VMEM((PAIRS * SLOT, LANES), f32),
            pltpu.VMEM((BLOCK, BLOCK), f32),
            pltpu.VMEM((BLOCK, BLOCK), f32),
            pltpu.SemaphoreType.DMA((2, 4)),
        ],
        compiler_params=pltpu.CompilerParams(vmem_limit_bytes=VMEM_LIMIT),
        name="apply",
    )(flag, got, *matrices)


def on_device(rho_real, rho_imag, gate_real, gate_imag, angles, targets, gate_order):
    flag = (lax.axis_index("row") == lax.axis_index("col")).astype(jnp.int32).reshape(1)
    sent = pack(flag, rho_real, rho_imag)
    got = lax.all_to_all(
        sent.reshape(PAIRS, 1, SLOT * LANES), ROW_COL, split_axis=0, concat_axis=0, tiled=True
    ).reshape(PAIRS * SLOT, LANES)
    matrices = gates(angles, targets, gate_order, gate_real, gate_imag)
    mixed_real, quadrature, purity = apply(flag, got, matrices)
    return mixed_real, quadrature, purity.reshape(())


def solution(mesh):
    placed = (P("row", "col"), P("row", "col"), P(), P(), P(), P(), P())
    return jax.shard_map(
        on_device,
        mesh=mesh,
        in_specs=placed,
        out_specs=(P("row", "col"), P("row", "col"), P()),
        check_vma=False,
    )
```

```python
import jax
import jax.numpy as jnp
from jax import lax
from jax.experimental import pallas as pl
from jax.experimental.pallas import tpu as pltpu
from jax.sharding import Mesh
from jax.sharding import PartitionSpec as P

LQ = 5
LOW = 2**LQ
GATE = 16
GATES = 8
DIM = 8192
ROW = ("row_0", "row_1", "row_2")
COL = ("col_0", "col_1")
ROW_COL = ROW + COL
RING = "col_0"

MIXING = 0.25
KEEP = 1 - MIXING

LANES = 128
SUB = 8
QUADS = LANES // LOW
BLOCK = GATE * LOW
PAIRS = GATE * GATE
SLOT = 2 * SUB
WIDE = 2 * LANES
HIGH_LOW = SUB.bit_length() - 1
highest = lax.Precision.HIGHEST
f32 = jnp.float32
bf16 = jnp.bfloat16
VMEM = pl.BlockSpec(memory_space=pltpu.VMEM)
SMEM = pl.BlockSpec(memory_space=pltpu.SMEM)
HBM = pl.BlockSpec(memory_space=pltpu.HBM)
VMEM_LIMIT = 16 * 1024 * 1024
VMEM_ALL = 67_043_328


def iota(shape, dim):
    return lax.broadcasted_iota(jnp.int32, shape, dim)


def swap_quads(parts):
    lane = iota((SUB, LANES), 1)
    low_half = lane < LANES // 2
    even = jnp.bitwise_and(lane, LOW) == 0
    half = [None] * QUADS
    for a in (0, 1):
        first, second = parts[a], parts[a + 2]
        moving = pltpu.roll(jnp.where(low_half, second, first), LANES // 2, 1)
        half[a] = jnp.where(low_half, first, moving)
        half[a + 2] = jnp.where(low_half, moving, second)
    out = [None] * QUADS
    for a in (0, 2):
        first, second = half[a], half[a + 1]
        out[a] = jnp.where(even, first, pltpu.roll(second, LOW, 1))
        out[a + 1] = jnp.where(even, pltpu.roll(first, LANES - LOW, 1), second)
    return out


def split(value):
    high = value.astype(bf16)
    return high, (value - high.astype(f32)).astype(bf16)


def dot(left, right):
    return jnp.dot(left, right, preferred_element_type=f32)


def three_pass(left, right):
    (left_high, left_low), (right_high, right_low) = left, right
    return dot(left_high, right_high) + dot(left_low, right_high) + dot(left_high, right_low)


CHUNKS = 8


def pack_kernel(flag_ref, real_hbm, imag_hbm, out_hbm, sums_ref, packed, real, imag, sems):
    rows = BLOCK // CHUNKS
    arriving = []
    for c in range(CHUNKS):
        at = pl.ds(c * rows, rows)
        pair = (
            pltpu.make_async_copy(real_hbm.at[at], real.at[at], sems.at[0, c]),
            pltpu.make_async_copy(imag_hbm.at[at], imag.at[at], sems.at[1, c]),
        )
        for copy in pair:
            copy.start()
        arriving.append(pair)
    squares = [jnp.zeros((SUB, LANES), f32) for _ in range(8)]
    diagonal = [jnp.zeros((SUB, LANES), f32) for _ in range(2)]
    leaving = []
    for c in range(CHUNKS):
        for copy in arriving[c]:
            copy.wait()
        for h in range(c * rows // LOW, (c + 1) * rows // LOW):
            for t in range(BLOCK // LANES):
                for part, ref in enumerate((real, imag)):
                    quads = [
                        ref[h * LOW + p * SUB : h * LOW + (p + 1) * SUB, t * LANES : (t + 1) * LANES]
                        for p in range(QUADS)
                    ]
                    for p, value in enumerate(quads):
                        squares[QUADS * part + p] += value * value
                    for q, value in enumerate(swap_quads(quads)):
                        slot = (h * GATE + t * QUADS + q) * SLOT
                        packed[slot + part * SUB : slot + (part + 1) * SUB, :] = value
        at = pl.ds(c * PAIRS * SLOT // CHUNKS, PAIRS * SLOT // CHUNKS)
        leaving.append(pltpu.make_async_copy(packed.at[at], out_hbm.at[at], sems.at[2, c]))
        leaving[-1].start()
        first = c * rows // LANES * LANES
        eye = iota((rows, LANES), 0) + (c * rows - first) == iota((rows, LANES), 1)
        for part, ref in enumerate((real, imag)):
            square = ref[c * rows : (c + 1) * rows, first : first + LANES]
            kept = jnp.where(eye, square, jnp.zeros_like(square))
            diagonal[part] += jnp.sum(kept.reshape(rows // SUB, SUB, LANES), axis=0)
    trace_real, trace_imag = (
        jnp.where(flag_ref[0] == 1, jnp.sum(value), 0.0) for value in diagonal
    )
    lane = iota((SUB, LANES), 1)
    total = jnp.where(lane == 2, jnp.sum(sum(squares)), 0.0)
    sums_ref[...] = jnp.where(lane == 0, trace_real, jnp.where(lane == 1, trace_imag, total))
    for copy in leaving:
        copy.wait()


def pack(flag, rho_real, rho_imag):
    return pl.pallas_call(
        pack_kernel,
        out_shape=[
            jax.ShapeDtypeStruct((PAIRS * SLOT, LANES), f32),
            jax.ShapeDtypeStruct((SUB, LANES), f32),
        ],
        in_specs=[SMEM, HBM, HBM],
        out_specs=[HBM, VMEM],
        scratch_shapes=[
            pltpu.VMEM((PAIRS * SLOT, LANES), f32),
            pltpu.VMEM((BLOCK, BLOCK), f32),
            pltpu.VMEM((BLOCK, BLOCK), f32),
            pltpu.SemaphoreType.DMA((3, CHUNKS)),
        ],
        compiler_params=pltpu.CompilerParams(vmem_limit_bytes=VMEM_ALL),
        name="pack",
    )(flag, rho_real, rho_imag)


def flip_rows(value, target):
    row = iota((LOW, LANES), 0)
    out = value
    for bit in range(LQ):
        step = 1 << bit
        up = pltpu.roll(value, LOW - step, 0)
        down = pltpu.roll(value, step, 0)
        flipped = jnp.where(jnp.bitwise_and(row, step) == 0, up, down)
        out = jnp.where(target == bit, flipped, out)
    return out


def factors_of(ref):
    return [
        tuple(ref.at[k * WIDE : (k + 1) * WIDE, half * WIDE : (half + 1) * WIDE] for half in range(2))
        for k in range(3)
    ]


def gates_kernel(angles_ref, targets_ref, order_ref, ur_ref, ui_ref, out_ref):
    row = iota((LOW, LANES), 0)
    lane = iota((LOW, LANES), 1)
    slot = iota((SUB, LANES), 0)
    half = jnp.zeros((SUB, LANES), f32)
    first = jnp.zeros((SUB, LANES), f32)
    second = jnp.zeros((SUB, LANES), f32)
    for k in range(GATES):
        gate = order_ref[k]
        half = jnp.where(slot == k, angles_ref[gate, 0], half)
        first = jnp.where(slot == k, angles_ref[gate, 1], first)
        second = jnp.where(slot == k, angles_ref[gate, 2], second)
    half = half / 2
    both = first + second
    c, s = jnp.cos(half), jnp.sin(half)
    entries = (
        (c, jnp.zeros_like(c)),
        (-jnp.cos(second) * s, -jnp.sin(second) * s),
        (jnp.cos(first) * s, jnp.sin(first) * s),
        (jnp.cos(both) * c, jnp.sin(both) * c),
    )
    unit = jnp.where(row == lane, 1.0, 0.0).astype(f32)
    products = [(unit, jnp.zeros_like(unit)), (unit, jnp.zeros_like(unit))]
    for k in range(GATES):
        target = targets_ref[order_ref[k]]
        high = jnp.bitwise_and(jnp.right_shift(row, target), 1) == 1
        low_low, low_high, high_low, high_high = (
            tuple(jnp.broadcast_to(member[k : k + 1, :], (LOW, LANES)) for member in entry)
            for entry in entries
        )
        same = [jnp.where(high, high_high[m], low_low[m]) for m in range(2)]
        other = [jnp.where(high, high_low[m], low_high[m]) for m in range(2)]
        for kind, (real, imag) in enumerate(products):
            flip_real = flip_rows(real, target)
            flip_imag = flip_rows(imag, target)
            new_real = same[0] * real - same[1] * imag + other[0] * flip_real - other[1] * flip_imag
            new_imag = same[0] * imag + same[1] * real + other[0] * flip_imag + other[1] * flip_real
            mine = (target < HIGH_LOW) == (kind == 0)
            products[kind] = (jnp.where(mine, new_real, real), jnp.where(mine, new_imag, imag))
    inner, outer = products

    def pick(size, index):
        return jnp.where(index(iota((LANES, size), 0)) == iota((LANES, size), 1), 1.0, 0.0).astype(f32)

    def expand(value, size, index):
        chosen = pick(size, index)

        def one(part):
            rows = jnp.dot(chosen, part, precision=highest, preferred_element_type=f32)
            return lax.dot_general(
                rows, chosen, (((1,), (1,)), ((), ())), precision=highest, preferred_element_type=f32
            )

        return tuple(one(part[:, :size]) for part in value)

    def times(left, right):
        return left[0] * right[0] - left[1] * right[1], left[0] * right[1] + left[1] * right[0]

    def conj(value):
        return value[0], -value[1]

    def transposed(value):
        return tuple(part[:, :LOW].T for part in value)

    flipped_inner, flipped_outer = transposed(inner), transposed(outer)
    group = expand(flipped_outer, LOW, lambda r: SUB * jnp.right_shift(r, LQ))
    own_high = expand(flipped_outer, LOW, lambda r: SUB * jnp.bitwise_and(jnp.right_shift(r, HIGH_LOW), QUADS - 1))
    own_sub = expand(flipped_inner, LOW, lambda r: jnp.bitwise_and(r, SUB - 1))
    right = times(group, conj(times(own_high, own_sub)))
    gate = (ur_ref[...], ui_ref[...])
    top = expand(gate, GATE, lambda r: jnp.right_shift(r, HIGH_LOW))
    sub = expand(inner, LOW, lambda r: jnp.bitwise_and(r, SUB - 1))
    rows_side = times(top, sub)
    same_sub = jnp.bitwise_and(iota((LANES, LANES), 0), SUB - 1) == jnp.bitwise_and(
        iota((LANES, LANES), 1), SUB - 1
    )
    cols_side = tuple(jnp.where(same_sub, KEEP * part, 0.0) for part in conj(top))

    refs = factors_of(out_ref)

    def place(which, at_row, at_col, value):
        for ref, part in zip(refs[which], split(value), strict=True):
            ref[at_row * LANES : (at_row + 1) * LANES, at_col * LANES : (at_col + 1) * LANES] = part

    for which, (real, imag), sign in ((0, right, -1), (1, rows_side, 1), (2, cols_side, 1)):
        place(which, 0, 0, real)
        place(which, 0, 1, -sign * imag)
        place(which, 1, 0, sign * imag)
        place(which, 1, 1, real)


def gates(angles, targets, gate_order, gate_real, gate_imag):
    return pl.pallas_call(
        gates_kernel,
        out_shape=jax.ShapeDtypeStruct((3 * WIDE, 2 * WIDE), bf16),
        in_specs=[SMEM, SMEM, SMEM, VMEM, VMEM],
        out_specs=VMEM,
        compiler_params=pltpu.CompilerParams(vmem_limit_bytes=VMEM_LIMIT),
        cost_estimate=pl.CostEstimate(flops=2_000_000_000, bytes_accessed=1_600_000, transcendentals=8192),
        name="gates",
    )(angles, targets, gate_order, gate_real, gate_imag)


def apply_kernel(
    flag_ref, sums_ref, got, factors, real_hbm, imag_hbm, purity_ref, first_done, second_done, real, imag, sems
):
    right, rows_side, cols_side = ([half[...] for half in pair] for pair in factors_of(factors))
    sums = sums_ref[0:1, :]
    lane = iota((1, LANES), 1)
    trace_real, trace_imag, squares = (jnp.sum(jnp.where(lane == k, sums, 0.0)) for k in range(3))
    purity_ref[0, 0] = (
        KEEP * KEEP * squares
        + (2 * KEEP * MIXING + MIXING * MIXING) * (trace_real * trace_real + trace_imag * trace_imag) / DIM
    ) / (DIM * DIM)
    shifts = [
        jnp.where(flag_ref[0] == 1, MIXING * trace / DIM, 0.0) for trace in (trace_real, trace_imag)
    ]

    for g in range(GATE):
        slots = got[g * GATE * SLOT : (g + 1) * GATE * SLOT, :].reshape(GATE, SLOT, LANES)
        value = jnp.concatenate(
            [slots[:, part * SUB : (part + 1) * SUB, :].reshape(LANES, LANES) for part in range(2)], axis=1
        )
        value = three_pass(split(value), right)
        for part in range(2):
            first_done[part, g] = value[:, part * LANES : (part + 1) * LANES].reshape(GATE, SUB, LANES)

    for g in range(0, GATE, 2):
        value = jnp.concatenate(
            [
                jnp.concatenate([first_done[part, :, g + k].reshape(LANES, LANES) for part in range(2)], axis=0)
                for k in range(2)
            ],
            axis=1,
        )
        value = three_pass(rows_side, split(value))
        for k in range(2):
            for part in range(2):
                second_done[part, :, g + k] = value[
                    part * LANES : (part + 1) * LANES, k * LANES : (k + 1) * LANES
                ].reshape(GATE, SUB, LANES)

    copies = []
    for g in range(0, GATE, 2):
        value = jnp.concatenate(
            [
                jnp.concatenate([second_done[part, g + k].reshape(LANES, LANES) for part in range(2)], axis=0)
                for k in range(2)
            ],
            axis=1,
        )
        value = three_pass(cols_side, split(value))
        for k in range(2):
            for part, ref in enumerate((real, imag)):
                block = value[part * LANES : (part + 1) * LANES, k * LANES : (k + 1) * LANES]
                for t in range(GATE // QUADS):
                    quads = swap_quads(
                        [block[(t * QUADS + q) * SUB : (t * QUADS + q + 1) * SUB, :] for q in range(QUADS)]
                    )
                    for p in range(QUADS):
                        at = (g + k) * LOW + p * SUB
                        out = quads[p]
                        if t == (g + k) // QUADS:
                            eye = iota((SUB, LANES), 0) + ((g + k) % QUADS * LOW + p * SUB) == iota((SUB, LANES), 1)
                            out = out + jnp.where(eye, shifts[part], 0.0)
                        ref[at : at + SUB, t * LANES : (t + 1) * LANES] = out
        at = pl.ds(g * LOW, 2 * LOW)
        for part, ref in enumerate((real, imag)):
            copy = pltpu.make_async_copy(ref.at[at], (real_hbm, imag_hbm)[part].at[at], sems.at[part, g // 2])
            copy.start()
            copies.append(copy)
    for copy in copies:
        copy.wait()


def apply(flag, sums, got, factors):
    return pl.pallas_call(
        apply_kernel,
        out_shape=[
            jax.ShapeDtypeStruct((BLOCK, BLOCK), f32),
            jax.ShapeDtypeStruct((BLOCK, BLOCK), f32),
            jax.ShapeDtypeStruct((1, 1), f32),
        ],
        in_specs=[SMEM, VMEM, VMEM, VMEM],
        out_specs=[HBM, HBM, SMEM],
        scratch_shapes=[
            pltpu.VMEM((2, GATE, GATE, SUB, LANES), f32),
            pltpu.VMEM((2, GATE, GATE, SUB, LANES), f32),
            pltpu.VMEM((BLOCK, BLOCK), f32),
            pltpu.VMEM((BLOCK, BLOCK), f32),
            pltpu.SemaphoreType.DMA((2, GATE // 2)),
        ],
        compiler_params=pltpu.CompilerParams(vmem_limit_bytes=VMEM_LIMIT),
        name="apply",
    )(flag, sums, got, factors)


def sum_everywhere(value):
    for axis in ROW_COL:
        if axis != RING:
            value = lax.psum(value, axis)
    size = lax.axis_size(RING)
    shifted = [
        lax.ppermute(value, RING, [(i, (i + k) % size) for i in range(size)]) for k in range(1, size)
    ]
    return value + sum(shifted)


def on_device(rho_real, rho_imag, gate_real, gate_imag, angles, targets, gate_order):
    flag = (lax.axis_index(ROW) == lax.axis_index(COL)).astype(jnp.int32).reshape(1)
    sent, sums = pack(flag, rho_real, rho_imag)
    got = lax.all_to_all(
        sent.reshape(PAIRS, 1, SLOT * LANES), ROW_COL, split_axis=0, concat_axis=0, tiled=True
    ).reshape(PAIRS * SLOT, LANES)
    sums = sum_everywhere(sums)
    factors = gates(angles, targets, gate_order, gate_real, gate_imag)
    mixed_real, quadrature, purity = apply(flag, sums, got, factors)
    return mixed_real, quadrature, purity.reshape(())


def solution(mesh):
    split_mesh = Mesh(mesh.devices.reshape(2, 4, 2, 8, 2), ROW_COL)
    placed = (P(ROW, COL), P(ROW, COL), P(), P(), P(), P(), P())
    return jax.shard_map(
        on_device,
        mesh=split_mesh,
        in_specs=placed,
        out_specs=(P(ROW, COL), P(ROW, COL), P()),
        check_vma=False,
    )
```

```python
import jax
import jax.numpy as jnp
from jax import lax
from jax.experimental import pallas as pl
from jax.experimental.pallas import tpu as pltpu
from jax.sharding import Mesh
from jax.sharding import PartitionSpec as P

LQ = 5
LOW = 2**LQ
GATE = 16
GATES = 8
DIM = 8192
ROW = ("row_0", "row_1", "row_2")
COL = ("col_0", "col_1")
ROW_COL = ROW + COL
RING = "col_0"

MIXING = 0.25
KEEP = 1 - MIXING

LANES = 128
SUB = 8
QUADS = LANES // LOW
BLOCK = GATE * LOW
PAIRS = GATE * GATE
SLOT = 2 * SUB
WIDE = 2 * LANES
HIGH_LOW = SUB.bit_length() - 1
highest = lax.Precision.HIGHEST
f32 = jnp.float32
bf16 = jnp.bfloat16
VMEM = pl.BlockSpec(memory_space=pltpu.VMEM)
SMEM = pl.BlockSpec(memory_space=pltpu.SMEM)
HBM = pl.BlockSpec(memory_space=pltpu.HBM)
VMEM_LIMIT = 16 * 1024 * 1024
VMEM_ALL = 67_043_328


def iota(shape, dim):
    return lax.broadcasted_iota(jnp.int32, shape, dim)


def swap_quads(parts):
    lane = iota((SUB, LANES), 1)
    low_half = lane < LANES // 2
    even = jnp.bitwise_and(lane, LOW) == 0
    outer = low_half == even

    def neighbours(first, second):
        moved = pltpu.roll(jnp.where(even, second, first), LOW, 1)
        return jnp.where(even, first, moved), jnp.where(even, moved, second)

    even_01, odd_01 = neighbours(parts[0], parts[1])
    even_23, odd_23 = neighbours(parts[2], parts[3])
    moved = pltpu.roll(jnp.where(low_half, even_23, even_01), LANES // 2, 1)
    turned = pltpu.roll(jnp.where(low_half, odd_23, odd_01), LANES // 2, 1)
    stay = jnp.where(low_half, odd_01, odd_23)
    return [
        jnp.where(low_half, even_01, moved),
        jnp.where(outer, turned, stay),
        jnp.where(low_half, moved, even_23),
        jnp.where(outer, stay, turned),
    ]


def split(value):
    high = value.astype(bf16)
    return high, (value - high.astype(f32)).astype(bf16)


def dot(left, right):
    return jnp.dot(left, right, preferred_element_type=f32)


def three_pass(left, right):
    (left_high, left_low), (right_high, right_low) = left, right
    return dot(left_high, right_high) + dot(left_low, right_high) + dot(left_high, right_low)


CHUNKS = 4


def pack_kernel(flag_ref, real_hbm, imag_hbm, out_hbm, sums_ref, packed, real, imag, sems):
    rows = BLOCK // CHUNKS
    arriving = []
    for c in range(CHUNKS):
        at = pl.ds(c * rows, rows)
        pair = (
            pltpu.make_async_copy(real_hbm.at[at], real.at[at], sems.at[0, c]),
            pltpu.make_async_copy(imag_hbm.at[at], imag.at[at], sems.at[1, c]),
        )
        for copy in pair:
            copy.start()
        arriving.append(pair)
    squares = [jnp.zeros((SUB, LANES), f32) for _ in range(8)]
    diagonal = [jnp.zeros((SUB, LANES), f32) for _ in range(2)]
    leaving = []
    for c in range(CHUNKS):
        for copy in arriving[c]:
            copy.wait()
        for h in range(c * rows // LOW, (c + 1) * rows // LOW):
            for t in range(BLOCK // LANES):
                for part, ref in enumerate((real, imag)):
                    quads = [
                        ref[h * LOW + p * SUB : h * LOW + (p + 1) * SUB, t * LANES : (t + 1) * LANES]
                        for p in range(QUADS)
                    ]
                    for p, value in enumerate(quads):
                        squares[QUADS * part + p] += value * value
                    for q, value in enumerate(swap_quads(quads)):
                        slot = (h * GATE + t * QUADS + q) * SLOT
                        packed[slot + part * SUB : slot + (part + 1) * SUB, :] = value
        at = pl.ds(c * PAIRS * SLOT // CHUNKS, PAIRS * SLOT // CHUNKS)
        leaving.append(pltpu.make_async_copy(packed.at[at], out_hbm.at[at], sems.at[2, c]))
        leaving[-1].start()
        first = c * rows // LANES * LANES
        eye = iota((rows, LANES), 0) + (c * rows - first) == iota((rows, LANES), 1)
        for part, ref in enumerate((real, imag)):
            square = ref[c * rows : (c + 1) * rows, first : first + LANES]
            kept = jnp.where(eye, square, jnp.zeros_like(square))
            diagonal[part] += jnp.sum(kept.reshape(rows // SUB, SUB, LANES), axis=0)
    trace_real, trace_imag = (
        jnp.where(flag_ref[0] == 1, jnp.sum(value), 0.0) for value in diagonal
    )
    lane = iota((1, LANES), 1)
    total = jnp.where(lane == 2, jnp.sum(sum(squares)), 0.0)
    sums_ref[...] = jnp.where(lane == 0, trace_real, jnp.where(lane == 1, trace_imag, total))
    for copy in leaving:
        copy.wait()


def pack(flag, rho_real, rho_imag):
    return pl.pallas_call(
        pack_kernel,
        out_shape=[
            jax.ShapeDtypeStruct((PAIRS * SLOT, LANES), f32),
            jax.ShapeDtypeStruct((1, LANES), f32),
        ],
        in_specs=[SMEM, HBM, HBM],
        out_specs=[HBM, VMEM],
        scratch_shapes=[
            pltpu.VMEM((PAIRS * SLOT, LANES), f32),
            pltpu.VMEM((BLOCK, BLOCK), f32),
            pltpu.VMEM((BLOCK, BLOCK), f32),
            pltpu.SemaphoreType.DMA((3, CHUNKS)),
        ],
        compiler_params=pltpu.CompilerParams(vmem_limit_bytes=VMEM_ALL),
        name="pack",
    )(flag, rho_real, rho_imag)


def flip_rows(value, target):
    row = iota((LOW, LANES), 0)
    out = value
    for bit in range(LQ):
        step = 1 << bit
        up = pltpu.roll(value, LOW - step, 0)
        down = pltpu.roll(value, step, 0)
        flipped = jnp.where(jnp.bitwise_and(row, step) == 0, up, down)
        out = jnp.where(target == bit, flipped, out)
    return out


def factors_of(ref):
    return [
        tuple(ref.at[k * WIDE : (k + 1) * WIDE, half * WIDE : (half + 1) * WIDE] for half in range(2))
        for k in range(3)
    ]


def gates_kernel(angles_ref, targets_ref, order_ref, ur_ref, ui_ref, out_ref):
    row = iota((LOW, LANES), 0)
    lane = iota((LOW, LANES), 1)
    slot = iota((SUB, LANES), 0)
    half = jnp.zeros((SUB, LANES), f32)
    first = jnp.zeros((SUB, LANES), f32)
    second = jnp.zeros((SUB, LANES), f32)
    for k in range(GATES):
        gate = order_ref[k]
        half = jnp.where(slot == k, angles_ref[gate, 0], half)
        first = jnp.where(slot == k, angles_ref[gate, 1], first)
        second = jnp.where(slot == k, angles_ref[gate, 2], second)
    half = half / 2
    both = first + second
    c, s = jnp.cos(half), jnp.sin(half)
    entries = (
        (c, jnp.zeros_like(c)),
        (-jnp.cos(second) * s, -jnp.sin(second) * s),
        (jnp.cos(first) * s, jnp.sin(first) * s),
        (jnp.cos(both) * c, jnp.sin(both) * c),
    )
    unit = jnp.where(row == lane, 1.0, 0.0).astype(f32)
    products = [(unit, jnp.zeros_like(unit)), (unit, jnp.zeros_like(unit))]
    for k in range(GATES):
        target = targets_ref[order_ref[k]]
        high = jnp.bitwise_and(jnp.right_shift(row, target), 1) == 1
        low_low, low_high, high_low, high_high = (
            tuple(jnp.broadcast_to(member[k : k + 1, :], (LOW, LANES)) for member in entry)
            for entry in entries
        )
        same = [jnp.where(high, high_high[m], low_low[m]) for m in range(2)]
        other = [jnp.where(high, high_low[m], low_high[m]) for m in range(2)]
        for kind, (real, imag) in enumerate(products):
            flip_real = flip_rows(real, target)
            flip_imag = flip_rows(imag, target)
            new_real = same[0] * real - same[1] * imag + other[0] * flip_real - other[1] * flip_imag
            new_imag = same[0] * imag + same[1] * real + other[0] * flip_imag + other[1] * flip_real
            mine = (target < HIGH_LOW) == (kind == 0)
            products[kind] = (jnp.where(mine, new_real, real), jnp.where(mine, new_imag, imag))
    inner, outer = products

    def pick(size, index):
        return jnp.where(index(iota((LANES, size), 0)) == iota((LANES, size), 1), 1.0, 0.0).astype(f32)

    def expand(value, size, index):
        chosen = pick(size, index)

        def one(part):
            rows = jnp.dot(chosen, part, precision=highest, preferred_element_type=f32)
            return lax.dot_general(
                rows, chosen, (((1,), (1,)), ((), ())), precision=highest, preferred_element_type=f32
            )

        return tuple(one(part[:, :size]) for part in value)

    def times(left, right):
        return left[0] * right[0] - left[1] * right[1], left[0] * right[1] + left[1] * right[0]

    def conj(value):
        return value[0], -value[1]

    def transposed(value):
        return tuple(part[:, :LOW].T for part in value)

    flipped_inner, flipped_outer = transposed(inner), transposed(outer)
    group = expand(flipped_outer, LOW, lambda r: SUB * jnp.right_shift(r, LQ))
    own_high = expand(flipped_outer, LOW, lambda r: SUB * jnp.bitwise_and(jnp.right_shift(r, HIGH_LOW), QUADS - 1))
    own_sub = expand(flipped_inner, LOW, lambda r: jnp.bitwise_and(r, SUB - 1))
    right = times(group, conj(times(own_high, own_sub)))
    gate = (ur_ref[...], ui_ref[...])
    top = expand(gate, GATE, lambda r: jnp.right_shift(r, HIGH_LOW))
    sub = expand(inner, LOW, lambda r: jnp.bitwise_and(r, SUB - 1))
    rows_side = times(top, sub)
    same_sub = jnp.bitwise_and(iota((LANES, LANES), 0), SUB - 1) == jnp.bitwise_and(
        iota((LANES, LANES), 1), SUB - 1
    )
    cols_side = tuple(jnp.where(same_sub, KEEP * part, 0.0) for part in conj(top))

    refs = factors_of(out_ref)

    def place(which, at_row, at_col, value):
        for ref, part in zip(refs[which], split(value), strict=True):
            ref[at_row * LANES : (at_row + 1) * LANES, at_col * LANES : (at_col + 1) * LANES] = part

    for which, (real, imag), sign in ((0, right, -1), (1, rows_side, 1), (2, cols_side, 1)):
        place(which, 0, 0, real)
        place(which, 0, 1, -sign * imag)
        place(which, 1, 0, sign * imag)
        place(which, 1, 1, real)


def gates(angles, targets, gate_order, gate_real, gate_imag):
    return pl.pallas_call(
        gates_kernel,
        out_shape=jax.ShapeDtypeStruct((3 * WIDE, 2 * WIDE), bf16),
        in_specs=[SMEM, SMEM, SMEM, VMEM, VMEM],
        out_specs=VMEM,
        compiler_params=pltpu.CompilerParams(vmem_limit_bytes=VMEM_LIMIT),
        cost_estimate=pl.CostEstimate(flops=2_000_000_000, bytes_accessed=1_600_000, transcendentals=8192),
        name="gates",
    )(angles, targets, gate_order, gate_real, gate_imag)


def apply_kernel(
    flag_ref, sums_ref, got, factors, real_hbm, imag_hbm, purity_ref, first_done, second_done, real, imag, sems
):
    right, rows_side, cols_side = ([half[...] for half in pair] for pair in factors_of(factors))
    sums = sums_ref[...]
    lane = iota((1, LANES), 1)
    trace_real, trace_imag, squares = (jnp.sum(jnp.where(lane == k, sums, 0.0)) for k in range(3))
    purity_ref[0, 0] = (
        KEEP * KEEP * squares
        + (2 * KEEP * MIXING + MIXING * MIXING) * (trace_real * trace_real + trace_imag * trace_imag) / DIM
    ) / (DIM * DIM)
    shifts = [
        jnp.where(flag_ref[0] == 1, MIXING * trace / DIM, 0.0) for trace in (trace_real, trace_imag)
    ]

    for g in range(GATE):
        slots = got[g * GATE * SLOT : (g + 1) * GATE * SLOT, :].reshape(GATE, SLOT, LANES)
        value = jnp.concatenate(
            [slots[:, part * SUB : (part + 1) * SUB, :].reshape(LANES, LANES) for part in range(2)], axis=1
        )
        value = three_pass(split(value), right)
        for part in range(2):
            first_done[part, g] = value[:, part * LANES : (part + 1) * LANES].reshape(GATE, SUB, LANES)

    for g in range(0, GATE, 2):
        value = jnp.concatenate(
            [
                jnp.concatenate([first_done[part, :, g + k].reshape(LANES, LANES) for part in range(2)], axis=0)
                for k in range(2)
            ],
            axis=1,
        )
        value = three_pass(rows_side, split(value))
        for k in range(2):
            for part in range(2):
                second_done[part, :, g + k] = value[
                    part * LANES : (part + 1) * LANES, k * LANES : (k + 1) * LANES
                ].reshape(GATE, SUB, LANES)

    copies = []
    for g in range(0, GATE, 2):
        value = jnp.concatenate(
            [
                jnp.concatenate([second_done[part, g + k].reshape(LANES, LANES) for part in range(2)], axis=0)
                for k in range(2)
            ],
            axis=1,
        )
        value = three_pass(cols_side, split(value))
        for k in range(2):
            for part, ref in enumerate((real, imag)):
                block = value[part * LANES : (part + 1) * LANES, k * LANES : (k + 1) * LANES]
                for t in range(GATE // QUADS):
                    quads = swap_quads(
                        [block[(t * QUADS + q) * SUB : (t * QUADS + q + 1) * SUB, :] for q in range(QUADS)]
                    )
                    for p in range(QUADS):
                        at = (g + k) * LOW + p * SUB
                        out = quads[p]
                        if t == (g + k) // QUADS:
                            eye = iota((SUB, LANES), 0) + ((g + k) % QUADS * LOW + p * SUB) == iota((SUB, LANES), 1)
                            out = out + jnp.where(eye, shifts[part], 0.0)
                        ref[at : at + SUB, t * LANES : (t + 1) * LANES] = out
        at = pl.ds(g * LOW, 2 * LOW)
        for part, ref in enumerate((real, imag)):
            copy = pltpu.make_async_copy(ref.at[at], (real_hbm, imag_hbm)[part].at[at], sems.at[part, g // 2])
            copy.start()
            copies.append(copy)
    for copy in copies:
        copy.wait()


def apply(flag, sums, got, factors):
    return pl.pallas_call(
        apply_kernel,
        out_shape=[
            jax.ShapeDtypeStruct((BLOCK, BLOCK), f32),
            jax.ShapeDtypeStruct((BLOCK, BLOCK), f32),
            jax.ShapeDtypeStruct((1, 1), f32),
        ],
        in_specs=[SMEM, VMEM, VMEM, VMEM],
        out_specs=[HBM, HBM, SMEM],
        scratch_shapes=[
            pltpu.VMEM((2, GATE, GATE, SUB, LANES), f32),
            pltpu.VMEM((2, GATE, GATE, SUB, LANES), f32),
            pltpu.VMEM((BLOCK, BLOCK), f32),
            pltpu.VMEM((BLOCK, BLOCK), f32),
            pltpu.SemaphoreType.DMA((2, GATE // 2)),
        ],
        compiler_params=pltpu.CompilerParams(vmem_limit_bytes=VMEM_LIMIT),
        name="apply",
    )(flag, sums, got, factors)


def sum_everywhere(value):
    for axis in ROW_COL:
        if axis != RING:
            value = lax.psum(value, axis)
    size = lax.axis_size(RING)
    shifted = [
        lax.ppermute(value, RING, [(i, (i + k) % size) for i in range(size)]) for k in range(1, size)
    ]
    return value + sum(shifted)


def on_device(rho_real, rho_imag, gate_real, gate_imag, angles, targets, gate_order):
    flag = (lax.axis_index(ROW) == lax.axis_index(COL)).astype(jnp.int32).reshape(1)
    sent, sums = pack(flag, rho_real, rho_imag)
    got = lax.all_to_all(
        sent.reshape(PAIRS, 1, SLOT * LANES), ROW_COL, split_axis=0, concat_axis=0, tiled=True
    ).reshape(PAIRS * SLOT, LANES)
    sums = sum_everywhere(sums)
    factors = gates(angles, targets, gate_order, gate_real, gate_imag)
    mixed_real, quadrature, purity = apply(flag, sums, got, factors)
    return mixed_real, quadrature, purity.reshape(())


def solution(mesh):
    split_mesh = Mesh(mesh.devices.reshape(2, 4, 2, 8, 2), ROW_COL)
    placed = (P(ROW, COL), P(ROW, COL), P(), P(), P(), P(), P())
    return jax.shard_map(
        on_device,
        mesh=split_mesh,
        in_specs=placed,
        out_specs=(P(ROW, COL), P(ROW, COL), P()),
        check_vma=False,
    )
```

```python
import jax
import jax.numpy as jnp
from jax import lax
from jax.experimental import pallas as pl
from jax.experimental.pallas import tpu as pltpu
from jax.sharding import Mesh
from jax.sharding import PartitionSpec as P

LQ = 5
LOW = 2**LQ
GATE = 16
GATES = 8
DIM = 8192
ROW = ("row_0", "row_1", "row_2")
COL = ("col_0", "col_1")
ROW_COL = ROW + COL
RING = "col_0"

MIXING = 0.25
KEEP = 1 - MIXING

LANES = 128
SUB = 8
QUADS = LANES // LOW
BLOCK = GATE * LOW
PAIRS = GATE * GATE
SLOT = 2 * SUB
WIDE = 2 * LANES
HIGH_LOW = SUB.bit_length() - 1
highest = lax.Precision.HIGHEST
f32 = jnp.float32
bf16 = jnp.bfloat16
VMEM = pl.BlockSpec(memory_space=pltpu.VMEM)
SMEM = pl.BlockSpec(memory_space=pltpu.SMEM)
HBM = pl.BlockSpec(memory_space=pltpu.HBM)
VMEM_LIMIT = 16 * 1024 * 1024
VMEM_ALL = 67_043_328


def iota(shape, dim):
    return lax.broadcasted_iota(jnp.int32, shape, dim)


def swap_quads(parts):
    lane = iota((SUB, LANES), 1)
    low_half = lane < LANES // 2
    even = jnp.bitwise_and(lane, LOW) == 0
    outer = low_half == even

    def neighbours(first, second):
        moved = pltpu.roll(jnp.where(even, second, first), LOW, 1)
        return jnp.where(even, first, moved), jnp.where(even, moved, second)

    even_01, odd_01 = neighbours(parts[0], parts[1])
    even_23, odd_23 = neighbours(parts[2], parts[3])
    moved = pltpu.roll(jnp.where(low_half, even_23, even_01), LANES // 2, 1)
    turned = pltpu.roll(jnp.where(low_half, odd_23, odd_01), LANES // 2, 1)
    stay = jnp.where(low_half, odd_01, odd_23)
    return [
        jnp.where(low_half, even_01, moved),
        jnp.where(outer, turned, stay),
        jnp.where(low_half, moved, even_23),
        jnp.where(outer, stay, turned),
    ]


def split(value):
    high = value.astype(bf16)
    return high, (value - high.astype(f32)).astype(bf16)


def dot(left, right):
    return jnp.dot(left, right, preferred_element_type=f32)


def three_pass(left, right):
    (left_high, left_low), (right_high, right_low) = left, right
    return dot(left_high, right_high) + dot(left_low, right_high) + dot(left_high, right_low)


CHUNKS = 4


def pack_kernel(flag_ref, real_hbm, imag_hbm, out_hbm, sums_hbm, packed, given, sums, arrive, leave, leave_sums):
    rows = BLOCK // CHUNKS
    sources = (real_hbm, imag_hbm)
    for c in range(CHUNKS):
        at = pl.ds(c * rows, rows)
        for part in range(2):
            pltpu.make_async_copy(sources[part].at[at], given.at[part, at], arrive.at[c]).start()
    squares = [jnp.zeros((SUB, LANES), f32) for _ in range(8)]
    diagonal = [jnp.zeros((SUB, LANES), f32) for _ in range(2)]
    for c in range(CHUNKS):
        both = given.at[:, pl.ds(c * rows, rows)]
        pltpu.make_async_copy(both, both, arrive.at[c]).wait()
        for h in range(c * rows // LOW, (c + 1) * rows // LOW):
            for t in range(BLOCK // LANES):
                for part in range(2):
                    quads = [
                        given[part, h * LOW + p * SUB : h * LOW + (p + 1) * SUB, t * LANES : (t + 1) * LANES]
                        for p in range(QUADS)
                    ]
                    for p, value in enumerate(quads):
                        squares[QUADS * part + p] += value * value
                    for q, value in enumerate(swap_quads(quads)):
                        slot = (h * GATE + t * QUADS + q) * SLOT
                        packed[slot + part * SUB : slot + (part + 1) * SUB, :] = value
        at = pl.ds(c * PAIRS * SLOT // CHUNKS, PAIRS * SLOT // CHUNKS)
        pltpu.make_async_copy(packed.at[at], out_hbm.at[at], leave).start()
        first = c * rows // LANES * LANES
        eye = iota((rows, LANES), 0) + (c * rows - first) == iota((rows, LANES), 1)
        for part in range(2):
            square = given[part, c * rows : (c + 1) * rows, first : first + LANES]
            kept = jnp.where(eye, square, jnp.zeros_like(square))
            diagonal[part] += jnp.sum(kept.reshape(rows // SUB, SUB, LANES), axis=0)

    def total(value):
        return jnp.sum(jnp.sum(value, axis=0, keepdims=True), axis=1, keepdims=True)

    lane = iota((1, LANES), 1)
    on_diagonal = flag_ref[0] == 1
    trace_real, trace_imag = (jnp.where(on_diagonal, total(value), 0.0) for value in diagonal)
    sums[...] = jnp.where(
        lane == 0,
        trace_real,
        jnp.where(lane == 1, trace_imag, jnp.where(lane == 2, total(sum(squares)), 0.0)),
    )
    leaving_sums = pltpu.make_async_copy(sums, sums_hbm, leave_sums)
    leaving_sums.start()
    pltpu.make_async_copy(packed, out_hbm, leave).wait()
    leaving_sums.wait()


def pack(flag, rho_real, rho_imag):
    return pl.pallas_call(
        pack_kernel,
        out_shape=[
            jax.ShapeDtypeStruct((PAIRS * SLOT, LANES), f32),
            jax.ShapeDtypeStruct((1, LANES), f32),
        ],
        in_specs=[SMEM, HBM, HBM],
        out_specs=[HBM, HBM],
        scratch_shapes=[
            pltpu.VMEM((PAIRS * SLOT, LANES), f32),
            pltpu.VMEM((2, BLOCK, BLOCK), f32),
            pltpu.VMEM((1, LANES), f32),
            pltpu.SemaphoreType.DMA((CHUNKS,)),
            pltpu.SemaphoreType.DMA,
            pltpu.SemaphoreType.DMA,
        ],
        compiler_params=pltpu.CompilerParams(vmem_limit_bytes=VMEM_ALL),
        name="pack",
    )(flag, rho_real, rho_imag)


def flip_rows(value, target):
    row = iota((LOW, LANES), 0)
    out = value
    for bit in range(LQ):
        step = 1 << bit
        up = pltpu.roll(value, LOW - step, 0)
        down = pltpu.roll(value, step, 0)
        flipped = jnp.where(jnp.bitwise_and(row, step) == 0, up, down)
        out = jnp.where(target == bit, flipped, out)
    return out


def factors_of(ref):
    return [
        tuple(ref.at[k * WIDE : (k + 1) * WIDE, half * WIDE : (half + 1) * WIDE] for half in range(2))
        for k in range(3)
    ]


def gates_kernel(angles_ref, targets_ref, order_ref, ur_ref, ui_ref, out_ref):
    row = iota((LOW, LANES), 0)
    lane = iota((LOW, LANES), 1)
    slot = iota((SUB, LANES), 0)
    half = jnp.zeros((SUB, LANES), f32)
    first = jnp.zeros((SUB, LANES), f32)
    second = jnp.zeros((SUB, LANES), f32)
    for k in range(GATES):
        gate = order_ref[k]
        half = jnp.where(slot == k, angles_ref[gate, 0], half)
        first = jnp.where(slot == k, angles_ref[gate, 1], first)
        second = jnp.where(slot == k, angles_ref[gate, 2], second)
    half = half / 2
    both = first + second
    c, s = jnp.cos(half), jnp.sin(half)
    entries = (
        (c, jnp.zeros_like(c)),
        (-jnp.cos(second) * s, -jnp.sin(second) * s),
        (jnp.cos(first) * s, jnp.sin(first) * s),
        (jnp.cos(both) * c, jnp.sin(both) * c),
    )
    unit = jnp.where(row == lane, 1.0, 0.0).astype(f32)
    products = [(unit, jnp.zeros_like(unit)), (unit, jnp.zeros_like(unit))]
    for k in range(GATES):
        target = targets_ref[order_ref[k]]
        high = jnp.bitwise_and(jnp.right_shift(row, target), 1) == 1
        low_low, low_high, high_low, high_high = (
            tuple(jnp.broadcast_to(member[k : k + 1, :], (LOW, LANES)) for member in entry)
            for entry in entries
        )
        same = [jnp.where(high, high_high[m], low_low[m]) for m in range(2)]
        other = [jnp.where(high, high_low[m], low_high[m]) for m in range(2)]
        for kind, (real, imag) in enumerate(products):
            flip_real = flip_rows(real, target)
            flip_imag = flip_rows(imag, target)
            new_real = same[0] * real - same[1] * imag + other[0] * flip_real - other[1] * flip_imag
            new_imag = same[0] * imag + same[1] * real + other[0] * flip_imag + other[1] * flip_real
            mine = (target < HIGH_LOW) == (kind == 0)
            products[kind] = (jnp.where(mine, new_real, real), jnp.where(mine, new_imag, imag))
    inner, outer = products

    def pick(size, index):
        return jnp.where(index(iota((LANES, size), 0)) == iota((LANES, size), 1), 1.0, 0.0).astype(f32)

    def expand(value, size, index):
        chosen = pick(size, index)

        def one(part):
            rows = jnp.dot(chosen, part, precision=highest, preferred_element_type=f32)
            return lax.dot_general(
                rows, chosen, (((1,), (1,)), ((), ())), precision=highest, preferred_element_type=f32
            )

        return tuple(one(part[:, :size]) for part in value)

    def times(left, right):
        return left[0] * right[0] - left[1] * right[1], left[0] * right[1] + left[1] * right[0]

    def conj(value):
        return value[0], -value[1]

    def transposed(value):
        return tuple(part[:, :LOW].T for part in value)

    flipped_inner, flipped_outer = transposed(inner), transposed(outer)
    group = expand(flipped_outer, LOW, lambda r: SUB * jnp.right_shift(r, LQ))
    own_high = expand(flipped_outer, LOW, lambda r: SUB * jnp.bitwise_and(jnp.right_shift(r, HIGH_LOW), QUADS - 1))
    own_sub = expand(flipped_inner, LOW, lambda r: jnp.bitwise_and(r, SUB - 1))
    right = times(group, conj(times(own_high, own_sub)))
    gate = (ur_ref[...], ui_ref[...])
    top = expand(gate, GATE, lambda r: jnp.right_shift(r, HIGH_LOW))
    sub = expand(inner, LOW, lambda r: jnp.bitwise_and(r, SUB - 1))
    rows_side = times(top, sub)
    same_sub = jnp.bitwise_and(iota((LANES, LANES), 0), SUB - 1) == jnp.bitwise_and(
        iota((LANES, LANES), 1), SUB - 1
    )
    cols_side = tuple(jnp.where(same_sub, KEEP * part, 0.0) for part in conj(top))

    refs = factors_of(out_ref)

    def place(which, at_row, at_col, value):
        for ref, part in zip(refs[which], split(value), strict=True):
            ref[at_row * LANES : (at_row + 1) * LANES, at_col * LANES : (at_col + 1) * LANES] = part

    for which, (real, imag), sign in ((0, right, -1), (1, rows_side, 1), (2, cols_side, 1)):
        place(which, 0, 0, real)
        place(which, 0, 1, -sign * imag)
        place(which, 1, 0, sign * imag)
        place(which, 1, 1, real)


def gates(angles, targets, gate_order, gate_real, gate_imag):
    return pl.pallas_call(
        gates_kernel,
        out_shape=jax.ShapeDtypeStruct((3 * WIDE, 2 * WIDE), bf16),
        in_specs=[SMEM, SMEM, SMEM, VMEM, VMEM],
        out_specs=VMEM,
        compiler_params=pltpu.CompilerParams(vmem_limit_bytes=VMEM_LIMIT),
        cost_estimate=pl.CostEstimate(flops=2_000_000_000, bytes_accessed=1_600_000, transcendentals=8192),
        name="gates",
    )(angles, targets, gate_order, gate_real, gate_imag)


def apply_kernel(
    flag_ref, sums_ref, got, factors, real_hbm, imag_hbm, purity_hbm,
    first_done, second_done, real, imag, purity, leave, leave_purity,
):
    right, rows_side, cols_side = ([half[...] for half in pair] for pair in factors_of(factors))
    sums = sums_ref[...]
    lane = iota((1, LANES), 1)
    trace_real, trace_imag, squares = (jnp.sum(jnp.where(lane == k, sums, 0.0)) for k in range(3))
    purity[0, 0] = (
        KEEP * KEEP * squares
        + (2 * KEEP * MIXING + MIXING * MIXING) * (trace_real * trace_real + trace_imag * trace_imag) / DIM
    ) / (DIM * DIM)
    leaving_purity = pltpu.make_async_copy(purity, purity_hbm, leave_purity)
    leaving_purity.start()
    shifts = [
        jnp.where(flag_ref[0] == 1, MIXING * trace / DIM, 0.0) for trace in (trace_real, trace_imag)
    ]

    for g in range(GATE):
        slots = got[g * GATE * SLOT : (g + 1) * GATE * SLOT, :].reshape(GATE, SLOT, LANES)
        value = jnp.concatenate(
            [slots[:, part * SUB : (part + 1) * SUB, :].reshape(LANES, LANES) for part in range(2)], axis=1
        )
        value = three_pass(split(value), right)
        for part in range(2):
            first_done[part, g] = value[:, part * LANES : (part + 1) * LANES].reshape(GATE, SUB, LANES)

    for g in range(0, GATE, 2):
        value = jnp.concatenate(
            [
                jnp.concatenate([first_done[part, :, g + k].reshape(LANES, LANES) for part in range(2)], axis=0)
                for k in range(2)
            ],
            axis=1,
        )
        value = three_pass(rows_side, split(value))
        for k in range(2):
            for part in range(2):
                second_done[part, :, g + k] = value[
                    part * LANES : (part + 1) * LANES, k * LANES : (k + 1) * LANES
                ].reshape(GATE, SUB, LANES)

    for g in range(0, GATE, 2):
        value = jnp.concatenate(
            [
                jnp.concatenate([second_done[part, g + k].reshape(LANES, LANES) for part in range(2)], axis=0)
                for k in range(2)
            ],
            axis=1,
        )
        value = three_pass(cols_side, split(value))
        for k in range(2):
            for part, ref in enumerate((real, imag)):
                block = value[part * LANES : (part + 1) * LANES, k * LANES : (k + 1) * LANES]
                for t in range(GATE // QUADS):
                    quads = swap_quads(
                        [block[(t * QUADS + q) * SUB : (t * QUADS + q + 1) * SUB, :] for q in range(QUADS)]
                    )
                    for p in range(QUADS):
                        at = (g + k) * LOW + p * SUB
                        out = quads[p]
                        if t == (g + k) // QUADS:
                            eye = iota((SUB, LANES), 0) + ((g + k) % QUADS * LOW + p * SUB) == iota((SUB, LANES), 1)
                            out = out + jnp.where(eye, shifts[part], 0.0)
                        ref[at : at + SUB, t * LANES : (t + 1) * LANES] = out
        at = pl.ds(g * LOW, 2 * LOW)
        for part, ref in enumerate((real, imag)):
            pltpu.make_async_copy(ref.at[at], (real_hbm, imag_hbm)[part].at[at], leave.at[part]).start()
    for part, ref in enumerate((real, imag)):
        pltpu.make_async_copy(ref, (real_hbm, imag_hbm)[part], leave.at[part]).wait()
    leaving_purity.wait()


def apply(flag, sums, got, factors):
    return pl.pallas_call(
        apply_kernel,
        out_shape=[
            jax.ShapeDtypeStruct((BLOCK, BLOCK), f32),
            jax.ShapeDtypeStruct((BLOCK, BLOCK), f32),
            jax.ShapeDtypeStruct((1, 1), f32),
        ],
        in_specs=[SMEM, VMEM, VMEM, VMEM],
        out_specs=[HBM, HBM, HBM],
        scratch_shapes=[
            pltpu.VMEM((2, GATE, GATE, SUB, LANES), f32),
            pltpu.VMEM((2, GATE, GATE, SUB, LANES), f32),
            pltpu.VMEM((BLOCK, BLOCK), f32),
            pltpu.VMEM((BLOCK, BLOCK), f32),
            pltpu.SMEM((1, 1), f32),
            pltpu.SemaphoreType.DMA((2,)),
            pltpu.SemaphoreType.DMA,
        ],
        compiler_params=pltpu.CompilerParams(vmem_limit_bytes=VMEM_LIMIT),
        name="apply",
    )(flag, sums, got, factors)


def sum_everywhere(value):
    for axis in ROW_COL:
        if axis != RING:
            value = lax.psum(value, axis)
    size = lax.axis_size(RING)
    shifted = [
        lax.ppermute(value, RING, [(i, (i + k) % size) for i in range(size)]) for k in range(1, size)
    ]
    return value + sum(shifted)


def on_device(rho_real, rho_imag, gate_real, gate_imag, angles, targets, gate_order):
    flag = (lax.axis_index(ROW) == lax.axis_index(COL)).astype(jnp.int32).reshape(1)
    sent, sums = pack(flag, rho_real, rho_imag)
    got = lax.all_to_all(
        sent.reshape(PAIRS, 1, SLOT * LANES), ROW_COL, split_axis=0, concat_axis=0, tiled=True
    ).reshape(PAIRS * SLOT, LANES)
    sums = sum_everywhere(sums)
    factors = gates(angles, targets, gate_order, gate_real, gate_imag)
    mixed_real, quadrature, purity = apply(flag, sums, got, factors)
    return mixed_real, quadrature, purity.reshape(())


def solution(mesh):
    split_mesh = Mesh(mesh.devices.reshape(2, 4, 2, 8, 2), ROW_COL)
    placed = (P(ROW, COL), P(ROW, COL), P(), P(), P(), P(), P())
    return jax.shard_map(
        on_device,
        mesh=split_mesh,
        in_specs=placed,
        out_specs=(P(ROW, COL), P(ROW, COL), P()),
        check_vma=False,
    )
```

```python
import jax
import jax.numpy as jnp
from jax import lax
from jax.experimental import pallas as pl
from jax.experimental.pallas import tpu as pltpu
from jax.sharding import Mesh
from jax.sharding import PartitionSpec as P

LQ = 5
LOW = 2**LQ
GATE = 16
GATES = 8
DIM = 8192
ROW = ("row_0", "row_1", "row_2")
COL = ("col_0", "col_1")
ROW_COL = ROW + COL
RING = "col_0"

MIXING = 0.25
KEEP = 1 - MIXING

LANES = 128
SUB = 8
QUADS = LANES // LOW
BLOCK = GATE * LOW
PAIRS = GATE * GATE
SLOT = 2 * SUB
WIDE = 2 * LANES
HIGH_LOW = SUB.bit_length() - 1
highest = lax.Precision.HIGHEST
f32 = jnp.float32
bf16 = jnp.bfloat16
VMEM = pl.BlockSpec(memory_space=pltpu.VMEM)
SMEM = pl.BlockSpec(memory_space=pltpu.SMEM)
HBM = pl.BlockSpec(memory_space=pltpu.HBM)
VMEM_LIMIT = 16 * 1024 * 1024
VMEM_ALL = 67_043_328


def iota(shape, dim):
    return lax.broadcasted_iota(jnp.int32, shape, dim)


def swap_quads(parts):
    lane = iota((SUB, LANES), 1)
    low_half = lane < LANES // 2
    even = jnp.bitwise_and(lane, LOW) == 0
    outer = low_half == even

    def neighbours(first, second):
        moved = pltpu.roll(jnp.where(even, second, first), LOW, 1)
        return jnp.where(even, first, moved), jnp.where(even, moved, second)

    even_01, odd_01 = neighbours(parts[0], parts[1])
    even_23, odd_23 = neighbours(parts[2], parts[3])
    moved = pltpu.roll(jnp.where(low_half, even_23, even_01), LANES // 2, 1)
    turned = pltpu.roll(jnp.where(low_half, odd_23, odd_01), LANES // 2, 1)
    stay = jnp.where(low_half, odd_01, odd_23)
    return [
        jnp.where(low_half, even_01, moved),
        jnp.where(outer, turned, stay),
        jnp.where(low_half, moved, even_23),
        jnp.where(outer, stay, turned),
    ]


def split(value):
    high = value.astype(bf16)
    return high, (value - high.astype(f32)).astype(bf16)


def dot(left, right):
    return jnp.dot(left, right, preferred_element_type=f32)


def three_pass(left, right):
    (left_high, left_low), (right_high, right_low) = left, right
    return dot(left_high, right_high) + dot(left_low, right_high) + dot(left_high, right_low)


CHUNKS = 4


def pack_kernel(flag_ref, real_hbm, imag_hbm, out_hbm, sums_hbm, packed, given, sums, arrive, leave, leave_sums):
    rows = BLOCK // CHUNKS
    sources = (real_hbm, imag_hbm)
    for c in range(CHUNKS):
        at = pl.ds(c * rows, rows)
        for part in range(2):
            pltpu.make_async_copy(sources[part].at[at], given.at[part, at], arrive.at[c]).start()
    squares = [jnp.zeros((SUB, LANES), f32) for _ in range(8)]
    diagonal = [jnp.zeros((SUB, LANES), f32) for _ in range(2)]
    for c in range(CHUNKS):
        both = given.at[:, pl.ds(c * rows, rows)]
        pltpu.make_async_copy(both, both, arrive.at[c]).wait()
        for h in range(c * rows // LOW, (c + 1) * rows // LOW):
            for t in range(BLOCK // LANES):
                for part in range(2):
                    quads = [
                        given[part, h * LOW + p * SUB : h * LOW + (p + 1) * SUB, t * LANES : (t + 1) * LANES]
                        for p in range(QUADS)
                    ]
                    for p, value in enumerate(quads):
                        squares[QUADS * part + p] += value * value
                    for q, value in enumerate(swap_quads(quads)):
                        slot = (h * GATE + t * QUADS + q) * SLOT
                        packed[slot + part * SUB : slot + (part + 1) * SUB, :] = value
        at = pl.ds(c * PAIRS * SLOT // CHUNKS, PAIRS * SLOT // CHUNKS)
        pltpu.make_async_copy(packed.at[at], out_hbm.at[at], leave).start()
        first = c * rows // LANES * LANES
        eye = iota((rows, LANES), 0) + (c * rows - first) == iota((rows, LANES), 1)
        for part in range(2):
            square = given[part, c * rows : (c + 1) * rows, first : first + LANES]
            kept = jnp.where(eye, square, jnp.zeros_like(square))
            diagonal[part] += jnp.sum(kept.reshape(rows // SUB, SUB, LANES), axis=0)

    def total(value):
        return jnp.sum(jnp.sum(value, axis=0, keepdims=True), axis=1, keepdims=True)

    lane = iota((1, LANES), 1)
    on_diagonal = flag_ref[0] == 1
    trace_real, trace_imag = (jnp.where(on_diagonal, total(value), 0.0) for value in diagonal)
    sums[...] = jnp.where(
        lane == 0,
        trace_real,
        jnp.where(lane == 1, trace_imag, jnp.where(lane == 2, total(sum(squares)), 0.0)),
    )
    leaving_sums = pltpu.make_async_copy(sums, sums_hbm, leave_sums)
    leaving_sums.start()
    pltpu.make_async_copy(packed, out_hbm, leave).wait()
    leaving_sums.wait()


def pack(flag, rho_real, rho_imag):
    return pl.pallas_call(
        pack_kernel,
        out_shape=[
            jax.ShapeDtypeStruct((PAIRS * SLOT, LANES), f32),
            jax.ShapeDtypeStruct((1, LANES), f32),
        ],
        in_specs=[SMEM, HBM, HBM],
        out_specs=[HBM, HBM],
        scratch_shapes=[
            pltpu.VMEM((PAIRS * SLOT, LANES), f32),
            pltpu.VMEM((2, BLOCK, BLOCK), f32),
            pltpu.VMEM((1, LANES), f32),
            pltpu.SemaphoreType.DMA((CHUNKS,)),
            pltpu.SemaphoreType.DMA,
            pltpu.SemaphoreType.DMA,
        ],
        compiler_params=pltpu.CompilerParams(vmem_limit_bytes=VMEM_ALL),
        name="pack",
    )(flag, rho_real, rho_imag)


def flip_rows(value, target):
    row = iota((LOW, LANES), 0)
    out = value
    for bit in range(LQ):
        step = 1 << bit
        up = pltpu.roll(value, LOW - step, 0)
        down = pltpu.roll(value, step, 0)
        flipped = jnp.where(jnp.bitwise_and(row, step) == 0, up, down)
        out = jnp.where(target == bit, flipped, out)
    return out


def factors_of(ref):
    return [
        tuple(ref.at[k * WIDE : (k + 1) * WIDE, half * WIDE : (half + 1) * WIDE] for half in range(2))
        for k in range(3)
    ]


def gates_kernel(angles_ref, targets_ref, order_ref, ur_ref, ui_ref, out_ref):
    row = iota((LOW, LANES), 0)
    lane = iota((LOW, LANES), 1)
    slot = iota((SUB, LANES), 0)
    half = jnp.zeros((SUB, LANES), f32)
    first = jnp.zeros((SUB, LANES), f32)
    second = jnp.zeros((SUB, LANES), f32)
    for k in range(GATES):
        gate = order_ref[k]
        half = jnp.where(slot == k, angles_ref[gate, 0], half)
        first = jnp.where(slot == k, angles_ref[gate, 1], first)
        second = jnp.where(slot == k, angles_ref[gate, 2], second)
    half = half / 2
    both = first + second
    c, s = jnp.cos(half), jnp.sin(half)
    entries = (
        (c, jnp.zeros_like(c)),
        (-jnp.cos(second) * s, -jnp.sin(second) * s),
        (jnp.cos(first) * s, jnp.sin(first) * s),
        (jnp.cos(both) * c, jnp.sin(both) * c),
    )
    unit = jnp.where(row == lane, 1.0, 0.0).astype(f32)
    products = [(unit, jnp.zeros_like(unit)), (unit, jnp.zeros_like(unit))]
    for k in range(GATES):
        target = targets_ref[order_ref[k]]
        high = jnp.bitwise_and(jnp.right_shift(row, target), 1) == 1
        low_low, low_high, high_low, high_high = (
            tuple(jnp.broadcast_to(member[k : k + 1, :], (LOW, LANES)) for member in entry)
            for entry in entries
        )
        same = [jnp.where(high, high_high[m], low_low[m]) for m in range(2)]
        other = [jnp.where(high, high_low[m], low_high[m]) for m in range(2)]
        for kind, (real, imag) in enumerate(products):
            flip_real = flip_rows(real, target)
            flip_imag = flip_rows(imag, target)
            new_real = same[0] * real - same[1] * imag + other[0] * flip_real - other[1] * flip_imag
            new_imag = same[0] * imag + same[1] * real + other[0] * flip_imag + other[1] * flip_real
            mine = (target < HIGH_LOW) == (kind == 0)
            products[kind] = (jnp.where(mine, new_real, real), jnp.where(mine, new_imag, imag))
    inner, outer = products

    def pick(size, index):
        return jnp.where(index(iota((LANES, size), 0)) == iota((LANES, size), 1), 1.0, 0.0).astype(f32)

    def expand(value, size, index):
        chosen = pick(size, index)

        def one(part):
            rows = jnp.dot(chosen, part, precision=highest, preferred_element_type=f32)
            return lax.dot_general(
                rows, chosen, (((1,), (1,)), ((), ())), precision=highest, preferred_element_type=f32
            )

        return tuple(one(part[:, :size]) for part in value)

    def times(left, right):
        return left[0] * right[0] - left[1] * right[1], left[0] * right[1] + left[1] * right[0]

    def conj(value):
        return value[0], -value[1]

    def transposed(value):
        return tuple(part[:, :LOW].T for part in value)

    flipped_inner, flipped_outer = transposed(inner), transposed(outer)
    group = expand(flipped_outer, LOW, lambda r: SUB * jnp.right_shift(r, LQ))
    own_high = expand(flipped_outer, LOW, lambda r: SUB * jnp.bitwise_and(jnp.right_shift(r, HIGH_LOW), QUADS - 1))
    own_sub = expand(flipped_inner, LOW, lambda r: jnp.bitwise_and(r, SUB - 1))
    right = times(group, conj(times(own_high, own_sub)))
    gate = (ur_ref[...], ui_ref[...])
    top = expand(gate, GATE, lambda r: jnp.right_shift(r, HIGH_LOW))
    sub = expand(inner, LOW, lambda r: jnp.bitwise_and(r, SUB - 1))
    rows_side = times(top, sub)
    same_sub = jnp.bitwise_and(iota((LANES, LANES), 0), SUB - 1) == jnp.bitwise_and(
        iota((LANES, LANES), 1), SUB - 1
    )
    cols_side = tuple(jnp.where(same_sub, KEEP * part, 0.0) for part in conj(top))

    refs = factors_of(out_ref)

    def place(which, at_row, at_col, value):
        for ref, part in zip(refs[which], split(value), strict=True):
            ref[at_row * LANES : (at_row + 1) * LANES, at_col * LANES : (at_col + 1) * LANES] = part

    for which, (real, imag), sign in ((0, right, -1), (1, rows_side, 1), (2, cols_side, 1)):
        place(which, 0, 0, real)
        place(which, 0, 1, -sign * imag)
        place(which, 1, 0, sign * imag)
        place(which, 1, 1, real)


def gates(angles, targets, gate_order, gate_real, gate_imag):
    return pl.pallas_call(
        gates_kernel,
        out_shape=jax.ShapeDtypeStruct((3 * WIDE, 2 * WIDE), bf16),
        in_specs=[SMEM, SMEM, SMEM, VMEM, VMEM],
        out_specs=VMEM,
        compiler_params=pltpu.CompilerParams(vmem_limit_bytes=VMEM_LIMIT),
        cost_estimate=pl.CostEstimate(flops=40_000_000, bytes_accessed=800_000, transcendentals=8192),
        name="gates",
    )(angles, targets, gate_order, gate_real, gate_imag)


def apply_kernel(
    flag_ref, sums_ref, got, factors, real_hbm, imag_hbm, purity_hbm,
    first_done, second_done, real, imag, purity, leave, leave_purity,
):
    right, rows_side, cols_side = ([half[...] for half in pair] for pair in factors_of(factors))
    sums = sums_ref[...]
    lane = iota((1, LANES), 1)
    trace_real, trace_imag, squares = (jnp.sum(jnp.where(lane == k, sums, 0.0)) for k in range(3))
    purity[0, 0] = (
        KEEP * KEEP * squares
        + (2 * KEEP * MIXING + MIXING * MIXING) * (trace_real * trace_real + trace_imag * trace_imag) / DIM
    ) / (DIM * DIM)
    leaving_purity = pltpu.make_async_copy(purity, purity_hbm, leave_purity)
    leaving_purity.start()
    shifts = [
        jnp.where(flag_ref[0] == 1, MIXING * trace / DIM, 0.0) for trace in (trace_real, trace_imag)
    ]

    for g in range(GATE):
        slots = got[g * GATE * SLOT : (g + 1) * GATE * SLOT, :].reshape(GATE, SLOT, LANES)
        value = jnp.concatenate(
            [slots[:, part * SUB : (part + 1) * SUB, :].reshape(LANES, LANES) for part in range(2)], axis=1
        )
        value = three_pass(split(value), right)
        for part in range(2):
            first_done[part, g] = value[:, part * LANES : (part + 1) * LANES].reshape(GATE, SUB, LANES)

    for g in range(0, GATE, 2):
        value = jnp.concatenate(
            [
                jnp.concatenate([first_done[part, :, g + k].reshape(LANES, LANES) for part in range(2)], axis=0)
                for k in range(2)
            ],
            axis=1,
        )
        value = three_pass(rows_side, split(value))
        for k in range(2):
            for part in range(2):
                second_done[part, :, g + k] = value[
                    part * LANES : (part + 1) * LANES, k * LANES : (k + 1) * LANES
                ].reshape(GATE, SUB, LANES)

    for g in range(0, GATE, 2):
        value = jnp.concatenate(
            [
                jnp.concatenate([second_done[part, g + k].reshape(LANES, LANES) for part in range(2)], axis=0)
                for k in range(2)
            ],
            axis=1,
        )
        value = three_pass(cols_side, split(value))
        for k in range(2):
            for part, ref in enumerate((real, imag)):
                block = value[part * LANES : (part + 1) * LANES, k * LANES : (k + 1) * LANES]
                for t in range(GATE // QUADS):
                    quads = swap_quads(
                        [block[(t * QUADS + q) * SUB : (t * QUADS + q + 1) * SUB, :] for q in range(QUADS)]
                    )
                    for p in range(QUADS):
                        at = (g + k) * LOW + p * SUB
                        out = quads[p]
                        if t == (g + k) // QUADS:
                            eye = iota((SUB, LANES), 0) + ((g + k) % QUADS * LOW + p * SUB) == iota((SUB, LANES), 1)
                            out = out + jnp.where(eye, shifts[part], 0.0)
                        ref[at : at + SUB, t * LANES : (t + 1) * LANES] = out
        at = pl.ds(g * LOW, 2 * LOW)
        for part, ref in enumerate((real, imag)):
            pltpu.make_async_copy(ref.at[at], (real_hbm, imag_hbm)[part].at[at], leave.at[part]).start()
    for part, ref in enumerate((real, imag)):
        pltpu.make_async_copy(ref, (real_hbm, imag_hbm)[part], leave.at[part]).wait()
    leaving_purity.wait()


def apply(flag, sums, got, factors):
    return pl.pallas_call(
        apply_kernel,
        out_shape=[
            jax.ShapeDtypeStruct((BLOCK, BLOCK), f32),
            jax.ShapeDtypeStruct((BLOCK, BLOCK), f32),
            jax.ShapeDtypeStruct((1, 1), f32),
        ],
        in_specs=[SMEM, VMEM, VMEM, VMEM],
        out_specs=[HBM, HBM, HBM],
        scratch_shapes=[
            pltpu.VMEM((2, GATE, GATE, SUB, LANES), f32),
            pltpu.VMEM((2, GATE, GATE, SUB, LANES), f32),
            pltpu.VMEM((BLOCK, BLOCK), f32),
            pltpu.VMEM((BLOCK, BLOCK), f32),
            pltpu.SMEM((1, 1), f32),
            pltpu.SemaphoreType.DMA((2,)),
            pltpu.SemaphoreType.DMA,
        ],
        compiler_params=pltpu.CompilerParams(vmem_limit_bytes=VMEM_LIMIT),
        name="apply",
    )(flag, sums, got, factors)


def sum_everywhere(value):
    for axis in ROW_COL:
        if axis != RING:
            value = lax.psum(value, axis)
    size = lax.axis_size(RING)
    shifted = [
        lax.ppermute(value, RING, [(i, (i + k) % size) for i in range(size)]) for k in range(1, size)
    ]
    return value + sum(shifted)


def on_device(rho_real, rho_imag, gate_real, gate_imag, angles, targets, gate_order):
    flag = (lax.axis_index(ROW) == lax.axis_index(COL)).astype(jnp.int32).reshape(1)
    sent, sums = pack(flag, rho_real, rho_imag)
    got = lax.all_to_all(
        sent.reshape(PAIRS, 1, SLOT * LANES), ROW_COL, split_axis=0, concat_axis=0, tiled=True
    ).reshape(PAIRS * SLOT, LANES)
    sums = sum_everywhere(sums)
    factors = gates(angles, targets, gate_order, gate_real, gate_imag)
    mixed_real, quadrature, purity = apply(flag, sums, got, factors)
    return mixed_real, quadrature, purity.reshape(())


def solution(mesh):
    split_mesh = Mesh(mesh.devices.reshape(2, 4, 2, 8, 2), ROW_COL)
    placed = (P(ROW, COL), P(ROW, COL), P(), P(), P(), P(), P())
    return jax.shard_map(
        on_device,
        mesh=split_mesh,
        in_specs=placed,
        out_specs=(P(ROW, COL), P(ROW, COL), P()),
        check_vma=False,
    )
```

```python
import jax
import jax.numpy as jnp
from jax import lax
from jax.experimental import pallas as pl
from jax.experimental.pallas import tpu as pltpu
from jax.sharding import Mesh
from jax.sharding import PartitionSpec as P

LQ = 5
LOW = 2**LQ
GATE = 16
GATES = 8
DIM = 8192
ROW = ("row_0", "row_1", "row_2")
COL = ("col_0", "col_1")
ROW_COL = ROW + COL
RING = "col_0"

MIXING = 0.25
KEEP = 1 - MIXING

LANES = 128
SUB = 8
QUADS = LANES // LOW
BLOCK = GATE * LOW
PAIRS = GATE * GATE
SLOT = 2 * SUB
WIDE = 2 * LANES
HIGH_LOW = SUB.bit_length() - 1
highest = lax.Precision.HIGHEST
f32 = jnp.float32
bf16 = jnp.bfloat16
VMEM = pl.BlockSpec(memory_space=pltpu.VMEM)
SMEM = pl.BlockSpec(memory_space=pltpu.SMEM)
HBM = pl.BlockSpec(memory_space=pltpu.HBM)
VMEM_LIMIT = 16 * 1024 * 1024
VMEM_ALL = 67_043_328


def iota(shape, dim):
    return lax.broadcasted_iota(jnp.int32, shape, dim)


def swap_quads(parts):
    lane = iota((SUB, LANES), 1)
    low_half = lane < LANES // 2
    even = jnp.bitwise_and(lane, LOW) == 0

    def turns(values):
        pairs = [jnp.where(even, values[k], values[(k + 1) % QUADS]) for k in range(QUADS)]
        return [jnp.where(low_half, pairs[k], pairs[(k + 2) % QUADS]) for k in range(QUADS)]

    moved = [pltpu.roll(v, k * LOW, 1) if k else v for k, v in enumerate(turns(parts))]
    out = turns(moved)
    return [out[-a % QUADS] for a in range(QUADS)]


def split(value):
    high = value.astype(bf16)
    return high, (value - high.astype(f32)).astype(bf16)


def dot(left, right):
    return jnp.dot(left, right, preferred_element_type=f32)


def three_pass(left, right):
    (left_high, left_low), (right_high, right_low) = left, right
    return dot(left_high, right_high) + dot(left_low, right_high) + dot(left_high, right_low)


CHUNKS = 4


def pack_kernel(flag_ref, real_hbm, imag_hbm, out_hbm, sums_hbm, packed, given, sums, arrive, leave, leave_sums):
    rows = BLOCK // CHUNKS
    sources = (real_hbm, imag_hbm)
    for c in range(CHUNKS):
        at = pl.ds(c * rows, rows)
        for part in range(2):
            pltpu.make_async_copy(sources[part].at[at], given.at[part, at], arrive.at[c]).start()
    squares = [jnp.zeros((SUB, LANES), f32) for _ in range(8)]
    diagonal = [jnp.zeros((SUB, LANES), f32) for _ in range(2)]
    for c in range(CHUNKS):
        both = given.at[:, pl.ds(c * rows, rows)]
        pltpu.make_async_copy(both, both, arrive.at[c]).wait()
        for h in range(c * rows // LOW, (c + 1) * rows // LOW):
            for t in range(BLOCK // LANES):
                for part in range(2):
                    quads = [
                        given[part, h * LOW + p * SUB : h * LOW + (p + 1) * SUB, t * LANES : (t + 1) * LANES]
                        for p in range(QUADS)
                    ]
                    for p, value in enumerate(quads):
                        squares[QUADS * part + p] += value * value
                    for q, value in enumerate(swap_quads(quads)):
                        slot = (h * GATE + t * QUADS + q) * SLOT
                        packed[slot + part * SUB : slot + (part + 1) * SUB, :] = value
        at = pl.ds(c * PAIRS * SLOT // CHUNKS, PAIRS * SLOT // CHUNKS)
        pltpu.make_async_copy(packed.at[at], out_hbm.at[at], leave).start()
        first = c * rows // LANES * LANES
        eye = iota((rows, LANES), 0) + (c * rows - first) == iota((rows, LANES), 1)
        for part in range(2):
            square = given[part, c * rows : (c + 1) * rows, first : first + LANES]
            kept = jnp.where(eye, square, jnp.zeros_like(square))
            diagonal[part] += jnp.sum(kept.reshape(rows // SUB, SUB, LANES), axis=0)

    def total(value):
        return jnp.sum(jnp.sum(value, axis=0, keepdims=True), axis=1, keepdims=True)

    lane = iota((1, LANES), 1)
    on_diagonal = flag_ref[0] == 1
    trace_real, trace_imag = (jnp.where(on_diagonal, total(value), 0.0) for value in diagonal)
    sums[...] = jnp.where(
        lane == 0,
        trace_real,
        jnp.where(lane == 1, trace_imag, jnp.where(lane == 2, total(sum(squares)), 0.0)),
    )
    leaving_sums = pltpu.make_async_copy(sums, sums_hbm, leave_sums)
    leaving_sums.start()
    pltpu.make_async_copy(packed, out_hbm, leave).wait()
    leaving_sums.wait()


def pack(flag, rho_real, rho_imag):
    return pl.pallas_call(
        pack_kernel,
        out_shape=[
            jax.ShapeDtypeStruct((PAIRS * SLOT, LANES), f32),
            jax.ShapeDtypeStruct((1, LANES), f32),
        ],
        in_specs=[SMEM, HBM, HBM],
        out_specs=[HBM, HBM],
        scratch_shapes=[
            pltpu.VMEM((PAIRS * SLOT, LANES), f32),
            pltpu.VMEM((2, BLOCK, BLOCK), f32),
            pltpu.VMEM((1, LANES), f32),
            pltpu.SemaphoreType.DMA((CHUNKS,)),
            pltpu.SemaphoreType.DMA,
            pltpu.SemaphoreType.DMA,
        ],
        compiler_params=pltpu.CompilerParams(vmem_limit_bytes=VMEM_ALL),
        name="pack",
    )(flag, rho_real, rho_imag)


def flip_rows(value, target):
    row = iota((LOW, LANES), 0)
    out = value
    for bit in range(LQ):
        step = 1 << bit
        up = pltpu.roll(value, LOW - step, 0)
        down = pltpu.roll(value, step, 0)
        flipped = jnp.where(jnp.bitwise_and(row, step) == 0, up, down)
        out = jnp.where(target == bit, flipped, out)
    return out


def factors_of(ref):
    return [
        tuple(ref.at[k * WIDE : (k + 1) * WIDE, half * WIDE : (half + 1) * WIDE] for half in range(2))
        for k in range(3)
    ]


def gates_kernel(angles_ref, targets_ref, order_ref, ur_ref, ui_ref, out_ref):
    row = iota((LOW, LANES), 0)
    lane = iota((LOW, LANES), 1)
    slot = iota((SUB, LANES), 0)
    half = jnp.zeros((SUB, LANES), f32)
    first = jnp.zeros((SUB, LANES), f32)
    second = jnp.zeros((SUB, LANES), f32)
    for k in range(GATES):
        gate = order_ref[k]
        half = jnp.where(slot == k, angles_ref[gate, 0], half)
        first = jnp.where(slot == k, angles_ref[gate, 1], first)
        second = jnp.where(slot == k, angles_ref[gate, 2], second)
    half = half / 2
    both = first + second
    c, s = jnp.cos(half), jnp.sin(half)
    entries = (
        (c, jnp.zeros_like(c)),
        (-jnp.cos(second) * s, -jnp.sin(second) * s),
        (jnp.cos(first) * s, jnp.sin(first) * s),
        (jnp.cos(both) * c, jnp.sin(both) * c),
    )
    unit = jnp.where(row == lane, 1.0, 0.0).astype(f32)
    products = [(unit, jnp.zeros_like(unit)), (unit, jnp.zeros_like(unit))]
    for k in range(GATES):
        target = targets_ref[order_ref[k]]
        high = jnp.bitwise_and(jnp.right_shift(row, target), 1) == 1
        low_low, low_high, high_low, high_high = (
            tuple(jnp.broadcast_to(member[k : k + 1, :], (LOW, LANES)) for member in entry)
            for entry in entries
        )
        same = [jnp.where(high, high_high[m], low_low[m]) for m in range(2)]
        other = [jnp.where(high, high_low[m], low_high[m]) for m in range(2)]
        for kind, (real, imag) in enumerate(products):
            flip_real = flip_rows(real, target)
            flip_imag = flip_rows(imag, target)
            new_real = same[0] * real - same[1] * imag + other[0] * flip_real - other[1] * flip_imag
            new_imag = same[0] * imag + same[1] * real + other[0] * flip_imag + other[1] * flip_real
            mine = (target < HIGH_LOW) == (kind == 0)
            products[kind] = (jnp.where(mine, new_real, real), jnp.where(mine, new_imag, imag))
    inner, outer = products

    def pick(size, index):
        return jnp.where(index(iota((LANES, size), 0)) == iota((LANES, size), 1), 1.0, 0.0).astype(f32)

    def expand(value, size, index):
        chosen = pick(size, index)

        def one(part):
            rows = jnp.dot(chosen, part, precision=highest, preferred_element_type=f32)
            return lax.dot_general(
                rows, chosen, (((1,), (1,)), ((), ())), precision=highest, preferred_element_type=f32
            )

        return tuple(one(part[:, :size]) for part in value)

    def times(left, right):
        return left[0] * right[0] - left[1] * right[1], left[0] * right[1] + left[1] * right[0]

    def conj(value):
        return value[0], -value[1]

    def transposed(value):
        return tuple(part[:, :LOW].T for part in value)

    flipped_inner, flipped_outer = transposed(inner), transposed(outer)
    group = expand(flipped_outer, LOW, lambda r: SUB * jnp.right_shift(r, LQ))
    own_high = expand(flipped_outer, LOW, lambda r: SUB * jnp.bitwise_and(jnp.right_shift(r, HIGH_LOW), QUADS - 1))
    own_sub = expand(flipped_inner, LOW, lambda r: jnp.bitwise_and(r, SUB - 1))
    right = times(group, conj(times(own_high, own_sub)))
    gate = (ur_ref[...], ui_ref[...])
    top = expand(gate, GATE, lambda r: jnp.right_shift(r, HIGH_LOW))
    sub = expand(inner, LOW, lambda r: jnp.bitwise_and(r, SUB - 1))
    rows_side = times(top, sub)
    same_sub = jnp.bitwise_and(iota((LANES, LANES), 0), SUB - 1) == jnp.bitwise_and(
        iota((LANES, LANES), 1), SUB - 1
    )
    cols_side = tuple(jnp.where(same_sub, KEEP * part, 0.0) for part in conj(top))

    refs = factors_of(out_ref)

    def place(which, at_row, at_col, value):
        for ref, part in zip(refs[which], split(value), strict=True):
            ref[at_row * LANES : (at_row + 1) * LANES, at_col * LANES : (at_col + 1) * LANES] = part

    for which, (real, imag), sign in ((0, right, -1), (1, rows_side, 1), (2, cols_side, 1)):
        place(which, 0, 0, real)
        place(which, 0, 1, -sign * imag)
        place(which, 1, 0, sign * imag)
        place(which, 1, 1, real)


def gates(angles, targets, gate_order, gate_real, gate_imag):
    return pl.pallas_call(
        gates_kernel,
        out_shape=jax.ShapeDtypeStruct((3 * WIDE, 2 * WIDE), bf16),
        in_specs=[SMEM, SMEM, SMEM, VMEM, VMEM],
        out_specs=VMEM,
        compiler_params=pltpu.CompilerParams(vmem_limit_bytes=VMEM_LIMIT),
        cost_estimate=pl.CostEstimate(flops=40_000_000, bytes_accessed=800_000, transcendentals=8192),
        name="gates",
    )(angles, targets, gate_order, gate_real, gate_imag)


def apply_kernel(
    flag_ref, sums_ref, got, factors, real_hbm, imag_hbm, purity_hbm,
    first_done, second_done, real, imag, purity, leave, leave_purity,
):
    right, rows_side, cols_side = ([half[...] for half in pair] for pair in factors_of(factors))
    sums = sums_ref[...]
    lane = iota((1, LANES), 1)
    trace_real, trace_imag, squares = (jnp.sum(jnp.where(lane == k, sums, 0.0)) for k in range(3))
    purity[0, 0] = (
        KEEP * KEEP * squares
        + (2 * KEEP * MIXING + MIXING * MIXING) * (trace_real * trace_real + trace_imag * trace_imag) / DIM
    ) / (DIM * DIM)
    leaving_purity = pltpu.make_async_copy(purity, purity_hbm, leave_purity)
    leaving_purity.start()
    shifts = [
        jnp.where(flag_ref[0] == 1, MIXING * trace / DIM, 0.0) for trace in (trace_real, trace_imag)
    ]

    for g in range(GATE):
        slots = got[g * GATE * SLOT : (g + 1) * GATE * SLOT, :].reshape(GATE, SLOT, LANES)
        value = jnp.concatenate(
            [slots[:, part * SUB : (part + 1) * SUB, :].reshape(LANES, LANES) for part in range(2)], axis=1
        )
        value = three_pass(split(value), right)
        for part in range(2):
            first_done[part, g] = value[:, part * LANES : (part + 1) * LANES].reshape(GATE, SUB, LANES)

    for g in range(0, GATE, 2):
        value = jnp.concatenate(
            [
                jnp.concatenate([first_done[part, :, g + k].reshape(LANES, LANES) for part in range(2)], axis=0)
                for k in range(2)
            ],
            axis=1,
        )
        value = three_pass(rows_side, split(value))
        for k in range(2):
            for part in range(2):
                second_done[part, :, g + k] = value[
                    part * LANES : (part + 1) * LANES, k * LANES : (k + 1) * LANES
                ].reshape(GATE, SUB, LANES)

    for g in range(0, GATE, 2):
        value = jnp.concatenate(
            [
                jnp.concatenate([second_done[part, g + k].reshape(LANES, LANES) for part in range(2)], axis=0)
                for k in range(2)
            ],
            axis=1,
        )
        value = three_pass(cols_side, split(value))
        for k in range(2):
            for part, ref in enumerate((real, imag)):
                block = value[part * LANES : (part + 1) * LANES, k * LANES : (k + 1) * LANES]
                for t in range(GATE // QUADS):
                    quads = swap_quads(
                        [block[(t * QUADS + q) * SUB : (t * QUADS + q + 1) * SUB, :] for q in range(QUADS)]
                    )
                    for p in range(QUADS):
                        at = (g + k) * LOW + p * SUB
                        out = quads[p]
                        if t == (g + k) // QUADS:
                            eye = iota((SUB, LANES), 0) + ((g + k) % QUADS * LOW + p * SUB) == iota((SUB, LANES), 1)
                            out = out + jnp.where(eye, shifts[part], 0.0)
                        ref[at : at + SUB, t * LANES : (t + 1) * LANES] = out
        at = pl.ds(g * LOW, 2 * LOW)
        for part, ref in enumerate((real, imag)):
            pltpu.make_async_copy(ref.at[at], (real_hbm, imag_hbm)[part].at[at], leave.at[part]).start()
    for part, ref in enumerate((real, imag)):
        pltpu.make_async_copy(ref, (real_hbm, imag_hbm)[part], leave.at[part]).wait()
    leaving_purity.wait()


def apply(flag, sums, got, factors):
    return pl.pallas_call(
        apply_kernel,
        out_shape=[
            jax.ShapeDtypeStruct((BLOCK, BLOCK), f32),
            jax.ShapeDtypeStruct((BLOCK, BLOCK), f32),
            jax.ShapeDtypeStruct((1, 1), f32),
        ],
        in_specs=[SMEM, VMEM, VMEM, VMEM],
        out_specs=[HBM, HBM, HBM],
        scratch_shapes=[
            pltpu.VMEM((2, GATE, GATE, SUB, LANES), f32),
            pltpu.VMEM((2, GATE, GATE, SUB, LANES), f32),
            pltpu.VMEM((BLOCK, BLOCK), f32),
            pltpu.VMEM((BLOCK, BLOCK), f32),
            pltpu.SMEM((1, 1), f32),
            pltpu.SemaphoreType.DMA((2,)),
            pltpu.SemaphoreType.DMA,
        ],
        compiler_params=pltpu.CompilerParams(vmem_limit_bytes=VMEM_LIMIT),
        name="apply",
    )(flag, sums, got, factors)


def sum_everywhere(value):
    for axis in ROW_COL:
        if axis != RING:
            value = lax.psum(value, axis)
    size = lax.axis_size(RING)
    shifted = [
        lax.ppermute(value, RING, [(i, (i + k) % size) for i in range(size)]) for k in range(1, size)
    ]
    return value + sum(shifted)


def on_device(rho_real, rho_imag, gate_real, gate_imag, angles, targets, gate_order):
    flag = (lax.axis_index(ROW) == lax.axis_index(COL)).astype(jnp.int32).reshape(1)
    sent, sums = pack(flag, rho_real, rho_imag)
    got = lax.all_to_all(
        sent.reshape(PAIRS, 1, SLOT * LANES), ROW_COL, split_axis=0, concat_axis=0, tiled=True
    ).reshape(PAIRS * SLOT, LANES)
    sums = sum_everywhere(sums)
    factors = gates(angles, targets, gate_order, gate_real, gate_imag)
    mixed_real, quadrature, purity = apply(flag, sums, got, factors)
    return mixed_real, quadrature, purity.reshape(())


def solution(mesh):
    split_mesh = Mesh(mesh.devices.reshape(2, 4, 2, 8, 2), ROW_COL)
    placed = (P(ROW, COL), P(ROW, COL), P(), P(), P(), P(), P())
    return jax.shard_map(
        on_device,
        mesh=split_mesh,
        in_specs=placed,
        out_specs=(P(ROW, COL), P(ROW, COL), P()),
        check_vma=False,
    )
```

```python
import jax
import jax.numpy as jnp
from jax import lax
from jax.experimental import pallas as pl
from jax.experimental.pallas import tpu as pltpu
from jax.sharding import Mesh
from jax.sharding import PartitionSpec as P

LQ = 5
LOW = 2**LQ
GATE = 16
GATES = 8
DIM = 8192
ROW = ("row_0", "row_1", "row_2")
COL = ("col_0", "col_1")
ROW_COL = ROW + COL
RING = "col_0"

MIXING = 0.25
KEEP = 1 - MIXING

LANES = 128
SUB = 8
QUADS = LANES // LOW
BLOCK = GATE * LOW
PAIRS = GATE * GATE
SLOT = 2 * SUB
WIDE = 2 * LANES
HIGH_LOW = SUB.bit_length() - 1
highest = lax.Precision.HIGHEST
f32 = jnp.float32
bf16 = jnp.bfloat16
VMEM = pl.BlockSpec(memory_space=pltpu.VMEM)
SMEM = pl.BlockSpec(memory_space=pltpu.SMEM)
HBM = pl.BlockSpec(memory_space=pltpu.HBM)
VMEM_LIMIT = 16 * 1024 * 1024
VMEM_ALL = 67_043_328


def iota(shape, dim):
    return lax.broadcasted_iota(jnp.int32, shape, dim)


def swap_quads(parts):
    lane = iota((SUB, LANES), 1)
    low_half = lane < LANES // 2
    even = jnp.bitwise_and(lane, LOW) == 0

    def turns(values):
        pairs = [jnp.where(even, values[k], values[(k + 1) % QUADS]) for k in range(QUADS)]
        return [jnp.where(low_half, pairs[k], pairs[(k + 2) % QUADS]) for k in range(QUADS)]

    moved = [pltpu.roll(v, k * LOW, 1) if k else v for k, v in enumerate(turns(parts))]
    out = turns(moved)
    return [out[-a % QUADS] for a in range(QUADS)]


def split(value):
    high = value.astype(bf16)
    return high, (value - high.astype(f32)).astype(bf16)


def dot(left, right):
    return jnp.dot(left, right, preferred_element_type=f32)


def three_pass(left, right):
    (left_high, left_low), (right_high, right_low) = left, right
    return dot(left_high, right_high) + dot(left_low, right_high) + dot(left_high, right_low)


CHUNKS = 4


def pack_kernel(flag_ref, real_hbm, imag_hbm, out_hbm, sums_hbm, packed, given, sums, arrive, leave, leave_sums):
    rows = BLOCK // CHUNKS
    sources = (real_hbm, imag_hbm)
    for c in range(CHUNKS):
        at = pl.ds(c * rows, rows)
        for part in range(2):
            pltpu.make_async_copy(sources[part].at[at], given.at[part, at], arrive.at[c]).start()
    squares = [jnp.zeros((SUB, LANES), f32) for _ in range(8)]
    diagonal = [jnp.zeros((SUB, LANES), f32) for _ in range(2)]
    for c in range(CHUNKS):
        both = given.at[:, pl.ds(c * rows, rows)]
        pltpu.make_async_copy(both, both, arrive.at[c]).wait()
        for h in range(c * rows // LOW, (c + 1) * rows // LOW):
            for t in range(BLOCK // LANES):
                for part in range(2):
                    quads = [
                        given[part, h * LOW + p * SUB : h * LOW + (p + 1) * SUB, t * LANES : (t + 1) * LANES]
                        for p in range(QUADS)
                    ]
                    for p, value in enumerate(quads):
                        squares[QUADS * part + p] += value * value
                    for q, value in enumerate(swap_quads(quads)):
                        slot = (h * GATE + t * QUADS + q) * SLOT
                        packed[slot + part * SUB : slot + (part + 1) * SUB, :] = value
        at = pl.ds(c * PAIRS * SLOT // CHUNKS, PAIRS * SLOT // CHUNKS)
        pltpu.make_async_copy(packed.at[at], out_hbm.at[at], leave).start()
        first = c * rows // LANES * LANES
        eye = iota((rows, LANES), 0) + (c * rows - first) == iota((rows, LANES), 1)
        for part in range(2):
            square = given[part, c * rows : (c + 1) * rows, first : first + LANES]
            kept = jnp.where(eye, square, jnp.zeros_like(square))
            diagonal[part] += jnp.sum(kept.reshape(rows // SUB, SUB, LANES), axis=0)

    def total(value):
        return jnp.sum(jnp.sum(value, axis=0, keepdims=True), axis=1, keepdims=True)

    lane = iota((1, LANES), 1)
    on_diagonal = flag_ref[0] == 1
    trace_real, trace_imag = (jnp.where(on_diagonal, total(value), 0.0) for value in diagonal)
    sums[...] = jnp.where(
        lane == 0,
        trace_real,
        jnp.where(lane == 1, trace_imag, jnp.where(lane == 2, total(sum(squares)), 0.0)),
    )
    leaving_sums = pltpu.make_async_copy(sums, sums_hbm, leave_sums)
    leaving_sums.start()
    pltpu.make_async_copy(packed, out_hbm, leave).wait()
    leaving_sums.wait()


def pack(flag, rho_real, rho_imag):
    return pl.pallas_call(
        pack_kernel,
        out_shape=[
            jax.ShapeDtypeStruct((PAIRS * SLOT, LANES), f32),
            jax.ShapeDtypeStruct((1, LANES), f32),
        ],
        in_specs=[SMEM, HBM, HBM],
        out_specs=[HBM, HBM],
        scratch_shapes=[
            pltpu.VMEM((PAIRS * SLOT, LANES), f32),
            pltpu.VMEM((2, BLOCK, BLOCK), f32),
            pltpu.VMEM((1, LANES), f32),
            pltpu.SemaphoreType.DMA((CHUNKS,)),
            pltpu.SemaphoreType.DMA,
            pltpu.SemaphoreType.DMA,
        ],
        compiler_params=pltpu.CompilerParams(vmem_limit_bytes=VMEM_ALL),
        name="pack",
    )(flag, rho_real, rho_imag)


def flip_rows(value, target):
    row = iota((LOW, LANES), 0)
    out = value
    for bit in range(LQ):
        step = 1 << bit
        up = pltpu.roll(value, LOW - step, 0)
        down = pltpu.roll(value, step, 0)
        flipped = jnp.where(jnp.bitwise_and(row, step) == 0, up, down)
        out = jnp.where(target == bit, flipped, out)
    return out


def factors_of(ref):
    return [
        tuple(ref.at[k * WIDE : (k + 1) * WIDE, half * WIDE : (half + 1) * WIDE] for half in range(2))
        for k in range(3)
    ]


def gates_kernel(angles_ref, targets_ref, order_ref, ur_ref, ui_ref, out_ref):
    row = iota((LOW, LANES), 0)
    lane = iota((LOW, LANES), 1)
    slot = iota((SUB, LANES), 0)
    half = jnp.zeros((SUB, LANES), f32)
    first = jnp.zeros((SUB, LANES), f32)
    second = jnp.zeros((SUB, LANES), f32)
    for k in range(GATES):
        gate = order_ref[k]
        half = jnp.where(slot == k, angles_ref[gate, 0], half)
        first = jnp.where(slot == k, angles_ref[gate, 1], first)
        second = jnp.where(slot == k, angles_ref[gate, 2], second)
    half = half / 2
    both = first + second
    c, s = jnp.cos(half), jnp.sin(half)
    entries = (
        (c, jnp.zeros_like(c)),
        (-jnp.cos(second) * s, -jnp.sin(second) * s),
        (jnp.cos(first) * s, jnp.sin(first) * s),
        (jnp.cos(both) * c, jnp.sin(both) * c),
    )
    unit = jnp.where(row == lane, 1.0, 0.0).astype(f32)
    products = [(unit, jnp.zeros_like(unit)), (unit, jnp.zeros_like(unit))]
    for k in range(GATES):
        target = targets_ref[order_ref[k]]
        high = jnp.bitwise_and(jnp.right_shift(row, target), 1) == 1
        low_low, low_high, high_low, high_high = (
            tuple(jnp.broadcast_to(member[k : k + 1, :], (LOW, LANES)) for member in entry)
            for entry in entries
        )
        same = [jnp.where(high, high_high[m], low_low[m]) for m in range(2)]
        other = [jnp.where(high, high_low[m], low_high[m]) for m in range(2)]
        for kind, (real, imag) in enumerate(products):
            flip_real = flip_rows(real, target)
            flip_imag = flip_rows(imag, target)
            new_real = same[0] * real - same[1] * imag + other[0] * flip_real - other[1] * flip_imag
            new_imag = same[0] * imag + same[1] * real + other[0] * flip_imag + other[1] * flip_real
            mine = (target < HIGH_LOW) == (kind == 0)
            products[kind] = (jnp.where(mine, new_real, real), jnp.where(mine, new_imag, imag))
    inner, outer = products

    def pick(size, index):
        return jnp.where(index(iota((LANES, size), 0)) == iota((LANES, size), 1), 1.0, 0.0).astype(f32)

    def expand(value, size, index):
        chosen = pick(size, index)

        def one(part):
            rows = jnp.dot(chosen, part, precision=highest, preferred_element_type=f32)
            return lax.dot_general(
                rows, chosen, (((1,), (1,)), ((), ())), precision=highest, preferred_element_type=f32
            )

        return tuple(one(part[:, :size]) for part in value)

    def times(left, right):
        return left[0] * right[0] - left[1] * right[1], left[0] * right[1] + left[1] * right[0]

    def conj(value):
        return value[0], -value[1]

    def transposed(value):
        return tuple(part[:, :LOW].T for part in value)

    flipped_inner, flipped_outer = transposed(inner), transposed(outer)
    group = expand(flipped_outer, LOW, lambda r: SUB * jnp.right_shift(r, LQ))
    own_high = expand(flipped_outer, LOW, lambda r: SUB * jnp.bitwise_and(jnp.right_shift(r, HIGH_LOW), QUADS - 1))
    own_sub = expand(flipped_inner, LOW, lambda r: jnp.bitwise_and(r, SUB - 1))
    right = times(group, conj(times(own_high, own_sub)))
    gate = (ur_ref[...], ui_ref[...])
    top = expand(gate, GATE, lambda r: jnp.right_shift(r, HIGH_LOW))
    sub = expand(inner, LOW, lambda r: jnp.bitwise_and(r, SUB - 1))
    rows_side = times(top, sub)
    same_sub = jnp.bitwise_and(iota((LANES, LANES), 0), SUB - 1) == jnp.bitwise_and(
        iota((LANES, LANES), 1), SUB - 1
    )
    cols_side = tuple(jnp.where(same_sub, KEEP * part, 0.0) for part in conj(top))

    refs = factors_of(out_ref)

    def place(which, at_row, at_col, value):
        for ref, part in zip(refs[which], split(value), strict=True):
            ref[at_row * LANES : (at_row + 1) * LANES, at_col * LANES : (at_col + 1) * LANES] = part

    for which, (real, imag), sign in ((0, right, -1), (1, rows_side, 1), (2, cols_side, 1)):
        place(which, 0, 0, real)
        place(which, 0, 1, -sign * imag)
        place(which, 1, 0, sign * imag)
        place(which, 1, 1, real)


def gates(angles, targets, gate_order, gate_real, gate_imag):
    return pl.pallas_call(
        gates_kernel,
        out_shape=jax.ShapeDtypeStruct((3 * WIDE, 2 * WIDE), bf16),
        in_specs=[SMEM, SMEM, SMEM, VMEM, VMEM],
        out_specs=VMEM,
        compiler_params=pltpu.CompilerParams(vmem_limit_bytes=VMEM_LIMIT),
        cost_estimate=pl.CostEstimate(flops=40_000_000, bytes_accessed=800_000, transcendentals=8192),
        name="gates",
    )(angles, targets, gate_order, gate_real, gate_imag)


def apply_kernel(
    flag_ref, sums_ref, got, factors, real_hbm, imag_hbm, purity_hbm,
    second_done, real, imag, purity, leave, leave_purity,
):
    right, rows_side, cols_side = ([half[...] for half in pair] for pair in factors_of(factors))
    slots = got.reshape(GATE, GATE, SLOT, LANES)

    def lanes_step(g, count):
        slot = slots[:, g : g + count]
        value = jnp.concatenate(
            [slot[:, :, part * SUB : (part + 1) * SUB, :].reshape(count * LANES, LANES) for part in range(2)], axis=1
        )
        value = three_pass(split(value), right).reshape(GATE, count, SUB, WIDE)
        return jnp.concatenate(
            [
                jnp.concatenate(
                    [value[:, k, :, part * LANES : (part + 1) * LANES].reshape(LANES, LANES) for part in range(2)], axis=0
                )
                for k in range(count)
            ],
            axis=1,
        )

    ready = lanes_step(0, 2)
    for g in range(0, GATE, 2):
        value = ready
        if g + 2 < GATE:
            ready = lanes_step(g + 2, 2)
        value = three_pass(rows_side, split(value))
        for k in range(2):
            for part in range(2):
                second_done[part, :, g + k] = value[
                    part * LANES : (part + 1) * LANES, k * LANES : (k + 1) * LANES
                ].reshape(GATE, SUB, LANES)

    sums = sums_ref[...]
    lane = iota((1, LANES), 1)
    trace_real, trace_imag, squares = (jnp.sum(jnp.where(lane == k, sums, 0.0)) for k in range(3))
    purity[0, 0] = (
        KEEP * KEEP * squares
        + (2 * KEEP * MIXING + MIXING * MIXING) * (trace_real * trace_real + trace_imag * trace_imag) / DIM
    ) / (DIM * DIM)
    leaving_purity = pltpu.make_async_copy(purity, purity_hbm, leave_purity)
    leaving_purity.start()
    shifts = [
        jnp.where(flag_ref[0] == 1, MIXING * trace / DIM, 0.0) for trace in (trace_real, trace_imag)
    ]

    for g in range(0, GATE, 2):
        value = jnp.concatenate(
            [
                jnp.concatenate([second_done[part, g + k].reshape(LANES, LANES) for part in range(2)], axis=0)
                for k in range(2)
            ],
            axis=1,
        )
        value = three_pass(cols_side, split(value))
        for k in range(2):
            for part, ref in enumerate((real, imag)):
                block = value[part * LANES : (part + 1) * LANES, k * LANES : (k + 1) * LANES]
                for t in range(GATE // QUADS):
                    quads = swap_quads(
                        [block[(t * QUADS + q) * SUB : (t * QUADS + q + 1) * SUB, :] for q in range(QUADS)]
                    )
                    for p in range(QUADS):
                        at = (g + k) * LOW + p * SUB
                        out = quads[p]
                        if t == (g + k) // QUADS:
                            eye = iota((SUB, LANES), 0) + ((g + k) % QUADS * LOW + p * SUB) == iota((SUB, LANES), 1)
                            out = out + jnp.where(eye, shifts[part], 0.0)
                        ref[at : at + SUB, t * LANES : (t + 1) * LANES] = out
        at = pl.ds(g * LOW, 2 * LOW)
        for part, ref in enumerate((real, imag)):
            pltpu.make_async_copy(ref.at[at], (real_hbm, imag_hbm)[part].at[at], leave.at[part]).start(priority=part)
    for part, ref in enumerate((real, imag)):
        pltpu.make_async_copy(ref, (real_hbm, imag_hbm)[part], leave.at[part]).wait()
    leaving_purity.wait()


def apply(flag, sums, got, factors):
    return pl.pallas_call(
        apply_kernel,
        out_shape=[
            jax.ShapeDtypeStruct((BLOCK, BLOCK), f32),
            jax.ShapeDtypeStruct((BLOCK, BLOCK), f32),
            jax.ShapeDtypeStruct((1, 1), f32),
        ],
        in_specs=[SMEM, VMEM, VMEM, VMEM],
        out_specs=[HBM, HBM, HBM],
        scratch_shapes=[
            pltpu.VMEM((2, GATE, GATE, SUB, LANES), f32),
            pltpu.VMEM((BLOCK, BLOCK), f32),
            pltpu.VMEM((BLOCK, BLOCK), f32),
            pltpu.SMEM((1, 1), f32),
            pltpu.SemaphoreType.DMA((2,)),
            pltpu.SemaphoreType.DMA,
        ],
        compiler_params=pltpu.CompilerParams(vmem_limit_bytes=VMEM_LIMIT),
        name="apply",
    )(flag, sums, got, factors)


def sum_everywhere(value):
    for axis in ROW_COL:
        if axis != RING:
            value = lax.psum(value, axis)
    size = lax.axis_size(RING)
    shifted = [
        lax.ppermute(value, RING, [(i, (i + k) % size) for i in range(size)]) for k in range(1, size)
    ]
    return value + sum(shifted)


def on_device(rho_real, rho_imag, gate_real, gate_imag, angles, targets, gate_order):
    flag = (lax.axis_index(ROW) == lax.axis_index(COL)).astype(jnp.int32).reshape(1)
    sent, sums = pack(flag, rho_real, rho_imag)
    got = lax.all_to_all(
        sent.reshape(PAIRS, 1, SLOT * LANES), ROW_COL, split_axis=0, concat_axis=0, tiled=True
    ).reshape(PAIRS * SLOT, LANES)
    sums = sum_everywhere(sums)
    factors = gates(angles, targets, gate_order, gate_real, gate_imag)
    mixed_real, quadrature, purity = apply(flag, sums, got, factors)
    return mixed_real, quadrature, purity.reshape(())


def solution(mesh):
    split_mesh = Mesh(mesh.devices.reshape(2, 4, 2, 8, 2), ROW_COL)
    placed = (P(ROW, COL), P(ROW, COL), P(), P(), P(), P(), P())
    return jax.shard_map(
        on_device,
        mesh=split_mesh,
        in_specs=placed,
        out_specs=(P(ROW, COL), P(ROW, COL), P()),
        check_vma=False,
    )
```

```python
import jax
import jax.numpy as jnp
from jax import lax
from jax.experimental import pallas as pl
from jax.experimental.pallas import tpu as pltpu
from jax.sharding import Mesh
from jax.sharding import PartitionSpec as P

LQ = 5
LOW = 2**LQ
GATE = 16
GATES = 8
DIM = 8192
ROW = ("row_0", "row_1", "row_2")
COL = ("col_0", "col_1")
ROW_COL = ROW + COL
RING = "col_0"

MIXING = 0.25
KEEP = 1 - MIXING

LANES = 128
SUB = 8
QUADS = LANES // LOW
BLOCK = GATE * LOW
PAIRS = GATE * GATE
SLOT = 2 * SUB
WIDE = 2 * LANES
HIGH_LOW = SUB.bit_length() - 1
highest = lax.Precision.HIGHEST
f32 = jnp.float32
bf16 = jnp.bfloat16
VMEM = pl.BlockSpec(memory_space=pltpu.VMEM)
SMEM = pl.BlockSpec(memory_space=pltpu.SMEM)
HBM = pl.BlockSpec(memory_space=pltpu.HBM)
VMEM_LIMIT = 16 * 1024 * 1024
VMEM_ALL = 67_043_328


def iota(shape, dim):
    return lax.broadcasted_iota(jnp.int32, shape, dim)


def swap_quads(parts):
    lane = iota((SUB, LANES), 1)
    low_half = lane < LANES // 2
    even = jnp.bitwise_and(lane, LOW) == 0

    def turns(values):
        pairs = [jnp.where(even, values[k], values[(k + 1) % QUADS]) for k in range(QUADS)]
        return [jnp.where(low_half, pairs[k], pairs[(k + 2) % QUADS]) for k in range(QUADS)]

    moved = [pltpu.roll(v, k * LOW, 1) if k else v for k, v in enumerate(turns(parts))]
    out = turns(moved)
    return [out[-a % QUADS] for a in range(QUADS)]


def split(value):
    high = value.astype(bf16)
    return high, (value - high.astype(f32)).astype(bf16)


def dot(left, right):
    return jnp.dot(left, right, preferred_element_type=f32)


def three_pass(left, right):
    (left_high, left_low), (right_high, right_low) = left, right
    return dot(left_high, right_high) + dot(left_low, right_high) + dot(left_high, right_low)


CHUNKS = 4


def pack_kernel(flag_ref, real_hbm, imag_hbm, out_hbm, sums_hbm, packed, given, sums, arrive, leave, leave_sums):
    rows = BLOCK // CHUNKS
    sources = (real_hbm, imag_hbm)
    for c in range(CHUNKS):
        at = pl.ds(c * rows, rows)
        for part in range(2):
            pltpu.make_async_copy(sources[part].at[at], given.at[part, at], arrive.at[c]).start()
    squares = [jnp.zeros((SUB, LANES), f32) for _ in range(8)]
    diagonal = [jnp.zeros((SUB, LANES), f32) for _ in range(2)]
    for c in range(CHUNKS):
        both = given.at[:, pl.ds(c * rows, rows)]
        pltpu.make_async_copy(both, both, arrive.at[c]).wait()
        for h in range(c * rows // LOW, (c + 1) * rows // LOW):
            for t in range(BLOCK // LANES):
                for part in range(2):
                    quads = [
                        given[part, h * LOW + p * SUB : h * LOW + (p + 1) * SUB, t * LANES : (t + 1) * LANES]
                        for p in range(QUADS)
                    ]
                    for p, value in enumerate(quads):
                        squares[QUADS * part + p] += value * value
                    for q, value in enumerate(swap_quads(quads)):
                        slot = (h * GATE + t * QUADS + q) * SLOT
                        packed[slot + part * SUB : slot + (part + 1) * SUB, :] = value
        at = pl.ds(c * PAIRS * SLOT // CHUNKS, PAIRS * SLOT // CHUNKS)
        pltpu.make_async_copy(packed.at[at], out_hbm.at[at], leave).start()
        first = c * rows // LANES * LANES
        eye = iota((rows, LANES), 0) + (c * rows - first) == iota((rows, LANES), 1)
        for part in range(2):
            square = given[part, c * rows : (c + 1) * rows, first : first + LANES]
            kept = jnp.where(eye, square, jnp.zeros_like(square))
            diagonal[part] += jnp.sum(kept.reshape(rows // SUB, SUB, LANES), axis=0)

    def total(value):
        return jnp.sum(jnp.sum(value, axis=0, keepdims=True), axis=1, keepdims=True)

    lane = iota((1, LANES), 1)
    on_diagonal = flag_ref[0] == 1
    trace_real, trace_imag = (jnp.where(on_diagonal, total(value), 0.0) for value in diagonal)
    sums[...] = jnp.where(
        lane == 0,
        trace_real,
        jnp.where(lane == 1, trace_imag, jnp.where(lane == 2, total(sum(squares)), 0.0)),
    )
    leaving_sums = pltpu.make_async_copy(sums, sums_hbm, leave_sums)
    leaving_sums.start()
    pltpu.make_async_copy(packed, out_hbm, leave).wait()
    leaving_sums.wait()


def pack(flag, rho_real, rho_imag):
    return pl.pallas_call(
        pack_kernel,
        out_shape=[
            jax.ShapeDtypeStruct((PAIRS * SLOT, LANES), f32),
            jax.ShapeDtypeStruct((1, LANES), f32),
        ],
        in_specs=[SMEM, HBM, HBM],
        out_specs=[HBM, HBM],
        scratch_shapes=[
            pltpu.VMEM((PAIRS * SLOT, LANES), f32),
            pltpu.VMEM((2, BLOCK, BLOCK), f32),
            pltpu.VMEM((1, LANES), f32),
            pltpu.SemaphoreType.DMA((CHUNKS,)),
            pltpu.SemaphoreType.DMA,
            pltpu.SemaphoreType.DMA,
        ],
        compiler_params=pltpu.CompilerParams(vmem_limit_bytes=VMEM_ALL),
        name="pack",
    )(flag, rho_real, rho_imag)


def flip_rows(value, target):
    row = iota((LOW, LANES), 0)
    out = value
    for bit in range(LQ):
        step = 1 << bit
        up = pltpu.roll(value, LOW - step, 0)
        down = pltpu.roll(value, step, 0)
        flipped = jnp.where(jnp.bitwise_and(row, step) == 0, up, down)
        out = jnp.where(target == bit, flipped, out)
    return out


def factors_of(ref):
    return [
        tuple(ref.at[k * WIDE : (k + 1) * WIDE, half * WIDE : (half + 1) * WIDE] for half in range(2))
        for k in range(3)
    ]


def gates_kernel(angles_ref, targets_ref, order_ref, ur_ref, ui_ref, out_ref):
    row = iota((LOW, LANES), 0)
    lane = iota((LOW, LANES), 1)
    slot = iota((SUB, LANES), 0)
    half = jnp.zeros((SUB, LANES), f32)
    first = jnp.zeros((SUB, LANES), f32)
    second = jnp.zeros((SUB, LANES), f32)
    for k in range(GATES):
        gate = order_ref[k]
        half = jnp.where(slot == k, angles_ref[gate, 0], half)
        first = jnp.where(slot == k, angles_ref[gate, 1], first)
        second = jnp.where(slot == k, angles_ref[gate, 2], second)
    half = half / 2
    both = first + second
    c, s = jnp.cos(half), jnp.sin(half)
    entries = (
        (c, jnp.zeros_like(c)),
        (-jnp.cos(second) * s, -jnp.sin(second) * s),
        (jnp.cos(first) * s, jnp.sin(first) * s),
        (jnp.cos(both) * c, jnp.sin(both) * c),
    )
    unit = jnp.where(row == lane, 1.0, 0.0).astype(f32)
    products = [(unit, jnp.zeros_like(unit)), (unit, jnp.zeros_like(unit))]
    for k in range(GATES):
        target = targets_ref[order_ref[k]]
        high = jnp.bitwise_and(jnp.right_shift(row, target), 1) == 1
        low_low, low_high, high_low, high_high = (
            tuple(jnp.broadcast_to(member[k : k + 1, :], (LOW, LANES)) for member in entry)
            for entry in entries
        )
        same = [jnp.where(high, high_high[m], low_low[m]) for m in range(2)]
        other = [jnp.where(high, high_low[m], low_high[m]) for m in range(2)]
        for kind, (real, imag) in enumerate(products):
            flip_real = flip_rows(real, target)
            flip_imag = flip_rows(imag, target)
            new_real = same[0] * real - same[1] * imag + other[0] * flip_real - other[1] * flip_imag
            new_imag = same[0] * imag + same[1] * real + other[0] * flip_imag + other[1] * flip_real
            mine = (target < HIGH_LOW) == (kind == 0)
            products[kind] = (jnp.where(mine, new_real, real), jnp.where(mine, new_imag, imag))
    inner, outer = products

    def pick(size, index):
        return jnp.where(index(iota((LANES, size), 0)) == iota((LANES, size), 1), 1.0, 0.0).astype(f32)

    def expand(value, size, index):
        chosen = pick(size, index)

        def one(part):
            rows = jnp.dot(chosen, part, precision=highest, preferred_element_type=f32)
            return lax.dot_general(
                rows, chosen, (((1,), (1,)), ((), ())), precision=highest, preferred_element_type=f32
            )

        return tuple(one(part[:, :size]) for part in value)

    def times(left, right):
        return left[0] * right[0] - left[1] * right[1], left[0] * right[1] + left[1] * right[0]

    def conj(value):
        return value[0], -value[1]

    def transposed(value):
        return tuple(part[:, :LOW].T for part in value)

    flipped_inner, flipped_outer = transposed(inner), transposed(outer)
    group = expand(flipped_outer, LOW, lambda r: SUB * jnp.right_shift(r, LQ))
    own_high = expand(flipped_outer, LOW, lambda r: SUB * jnp.bitwise_and(jnp.right_shift(r, HIGH_LOW), QUADS - 1))
    own_sub = expand(flipped_inner, LOW, lambda r: jnp.bitwise_and(r, SUB - 1))
    right = times(group, conj(times(own_high, own_sub)))
    gate = (ur_ref[...], ui_ref[...])
    top = expand(gate, GATE, lambda r: jnp.right_shift(r, HIGH_LOW))
    sub = expand(inner, LOW, lambda r: jnp.bitwise_and(r, SUB - 1))
    rows_side = times(top, sub)
    same_sub = jnp.bitwise_and(iota((LANES, LANES), 0), SUB - 1) == jnp.bitwise_and(
        iota((LANES, LANES), 1), SUB - 1
    )
    cols_side = tuple(jnp.where(same_sub, KEEP * part, 0.0) for part in conj(top))

    refs = factors_of(out_ref)

    def place(which, at_row, at_col, value):
        for ref, part in zip(refs[which], split(value), strict=True):
            ref[at_row * LANES : (at_row + 1) * LANES, at_col * LANES : (at_col + 1) * LANES] = part

    for which, (real, imag), sign in ((0, right, -1), (1, rows_side, 1), (2, cols_side, 1)):
        place(which, 0, 0, real)
        place(which, 0, 1, -sign * imag)
        place(which, 1, 0, sign * imag)
        place(which, 1, 1, real)


def gates(angles, targets, gate_order, gate_real, gate_imag):
    return pl.pallas_call(
        gates_kernel,
        out_shape=jax.ShapeDtypeStruct((3 * WIDE, 2 * WIDE), bf16),
        in_specs=[SMEM, SMEM, SMEM, VMEM, VMEM],
        out_specs=VMEM,
        compiler_params=pltpu.CompilerParams(vmem_limit_bytes=VMEM_LIMIT),
        cost_estimate=pl.CostEstimate(flops=40_000_000, bytes_accessed=800_000, transcendentals=8192),
        name="gates",
    )(angles, targets, gate_order, gate_real, gate_imag)


def apply_kernel(
    flag_ref, sums_ref, got, factors, real_hbm, imag_hbm, purity_hbm,
    first_done, second_done, real, imag, purity, leave, leave_purity,
):
    right, rows_side, cols_side = ([half[...] for half in pair] for pair in factors_of(factors))
    sums = sums_ref[...]
    lane = iota((1, LANES), 1)
    trace_real, trace_imag, squares = (jnp.sum(jnp.where(lane == k, sums, 0.0)) for k in range(3))
    purity[0, 0] = (
        KEEP * KEEP * squares
        + (2 * KEEP * MIXING + MIXING * MIXING) * (trace_real * trace_real + trace_imag * trace_imag) / DIM
    ) / (DIM * DIM)
    leaving_purity = pltpu.make_async_copy(purity, purity_hbm, leave_purity)
    leaving_purity.start()
    shifts = [
        jnp.where(flag_ref[0] == 1, MIXING * trace / DIM, 0.0) for trace in (trace_real, trace_imag)
    ]

    for g in range(GATE):
        slots = got[g * GATE * SLOT : (g + 1) * GATE * SLOT, :].reshape(GATE, SLOT, LANES)
        value = jnp.concatenate(
            [slots[:, part * SUB : (part + 1) * SUB, :].reshape(LANES, LANES) for part in range(2)], axis=1
        )
        value = three_pass(split(value), right)
        for part in range(2):
            first_done[part, g] = value[:, part * LANES : (part + 1) * LANES].reshape(GATE, SUB, LANES)

    for g in range(0, GATE, 2):
        value = jnp.concatenate(
            [
                jnp.concatenate([first_done[part, :, g + k].reshape(LANES, LANES) for part in range(2)], axis=0)
                for k in range(2)
            ],
            axis=1,
        )
        value = three_pass(rows_side, split(value))
        for k in range(2):
            for part in range(2):
                second_done[part, :, g + k] = value[
                    part * LANES : (part + 1) * LANES, k * LANES : (k + 1) * LANES
                ].reshape(GATE, SUB, LANES)

    for g in range(0, GATE, 2):
        value = jnp.concatenate(
            [
                jnp.concatenate([second_done[part, g + k].reshape(LANES, LANES) for part in range(2)], axis=0)
                for k in range(2)
            ],
            axis=1,
        )
        value = three_pass(cols_side, split(value))
        for k in range(2):
            for part, ref in enumerate((real, imag)):
                block = value[part * LANES : (part + 1) * LANES, k * LANES : (k + 1) * LANES]
                for t in range(GATE // QUADS):
                    quads = swap_quads(
                        [block[(t * QUADS + q) * SUB : (t * QUADS + q + 1) * SUB, :] for q in range(QUADS)]
                    )
                    for p in range(QUADS):
                        at = (g + k) * LOW + p * SUB
                        out = quads[p]
                        if t == (g + k) // QUADS:
                            eye = iota((SUB, LANES), 0) + ((g + k) % QUADS * LOW + p * SUB) == iota((SUB, LANES), 1)
                            out = out + jnp.where(eye, shifts[part], 0.0)
                        ref[at : at + SUB, t * LANES : (t + 1) * LANES] = out
        at = pl.ds(g * LOW, 2 * LOW)
        for part, ref in enumerate((real, imag)):
            pltpu.make_async_copy(ref.at[at], (real_hbm, imag_hbm)[part].at[at], leave.at[part]).start()
    for part, ref in enumerate((real, imag)):
        pltpu.make_async_copy(ref, (real_hbm, imag_hbm)[part], leave.at[part]).wait()
    leaving_purity.wait()


def apply(flag, sums, got, factors):
    return pl.pallas_call(
        apply_kernel,
        out_shape=[
            jax.ShapeDtypeStruct((BLOCK, BLOCK), f32),
            jax.ShapeDtypeStruct((BLOCK, BLOCK), f32),
            jax.ShapeDtypeStruct((1, 1), f32),
        ],
        in_specs=[SMEM, VMEM, VMEM, VMEM],
        out_specs=[HBM, HBM, HBM],
        scratch_shapes=[
            pltpu.VMEM((2, GATE, GATE, SUB, LANES), f32),
            pltpu.VMEM((2, GATE, GATE, SUB, LANES), f32),
            pltpu.VMEM((BLOCK, BLOCK), f32),
            pltpu.VMEM((BLOCK, BLOCK), f32),
            pltpu.SMEM((1, 1), f32),
            pltpu.SemaphoreType.DMA((2,)),
            pltpu.SemaphoreType.DMA,
        ],
        compiler_params=pltpu.CompilerParams(vmem_limit_bytes=VMEM_LIMIT),
        name="apply",
    )(flag, sums, got, factors)


def sum_everywhere(value):
    for axis in ROW_COL:
        if axis != RING:
            value = lax.psum(value, axis)
    size = lax.axis_size(RING)
    shifted = [
        lax.ppermute(value, RING, [(i, (i + k) % size) for i in range(size)]) for k in range(1, size)
    ]
    return value + sum(shifted)


def on_device(rho_real, rho_imag, gate_real, gate_imag, angles, targets, gate_order):
    flag = (lax.axis_index(ROW) == lax.axis_index(COL)).astype(jnp.int32).reshape(1)
    sent, sums = pack(flag, rho_real, rho_imag)
    got = lax.all_to_all(
        sent.reshape(PAIRS, 1, SLOT * LANES), ROW_COL, split_axis=0, concat_axis=0, tiled=True
    ).reshape(PAIRS * SLOT, LANES)
    factors = gates(angles, targets, gate_order, gate_real, gate_imag)
    sums, factors = lax.optimization_barrier((sums, factors))
    sums = sum_everywhere(sums)
    mixed_real, quadrature, purity = apply(flag, sums, got, factors)
    return mixed_real, quadrature, purity.reshape(())


def solution(mesh):
    split_mesh = Mesh(mesh.devices.reshape(2, 4, 2, 8, 2), ROW_COL)
    placed = (P(ROW, COL), P(ROW, COL), P(), P(), P(), P(), P())
    return jax.shard_map(
        on_device,
        mesh=split_mesh,
        in_specs=placed,
        out_specs=(P(ROW, COL), P(ROW, COL), P()),
        check_vma=False,
    )
```

```python
import jax
import jax.numpy as jnp
from jax import lax
from jax.experimental import pallas as pl
from jax.experimental.pallas import tpu as pltpu
from jax.sharding import Mesh
from jax.sharding import PartitionSpec as P

LQ = 5
LOW = 2**LQ
GATE = 16
GATES = 8
DIM = 8192
ROW = ("row_0", "row_1", "row_2")
COL = ("col_0", "col_1")
ROW_COL = ROW + COL
RING = "col_0"

MIXING = 0.25
KEEP = 1 - MIXING

LANES = 128
SUB = 8
QUADS = LANES // LOW
BLOCK = GATE * LOW
PAIRS = GATE * GATE
SLOT = 2 * SUB
WIDE = 2 * LANES
HIGH_LOW = SUB.bit_length() - 1
highest = lax.Precision.HIGHEST
f32 = jnp.float32
bf16 = jnp.bfloat16
VMEM = pl.BlockSpec(memory_space=pltpu.VMEM)
SMEM = pl.BlockSpec(memory_space=pltpu.SMEM)
HBM = pl.BlockSpec(memory_space=pltpu.HBM)
VMEM_LIMIT = 16 * 1024 * 1024
VMEM_ALL = 67_043_328


def iota(shape, dim):
    return lax.broadcasted_iota(jnp.int32, shape, dim)


def swap_quads(parts):
    lane = iota((SUB, LANES), 1)
    low_half = lane < LANES // 2
    even = jnp.bitwise_and(lane, LOW) == 0

    def turns(values):
        pairs = [jnp.where(even, values[k], values[(k + 1) % QUADS]) for k in range(QUADS)]
        return [jnp.where(low_half, pairs[k], pairs[(k + 2) % QUADS]) for k in range(QUADS)]

    moved = [pltpu.roll(v, k * LOW, 1) if k else v for k, v in enumerate(turns(parts))]
    out = turns(moved)
    return [out[-a % QUADS] for a in range(QUADS)]


def split(value):
    high = value.astype(bf16)
    return high, (value - high.astype(f32)).astype(bf16)


def dot(left, right):
    return jnp.dot(left, right, preferred_element_type=f32)


def three_pass(left, right):
    (left_high, left_low), (right_high, right_low) = left, right
    return dot(left_high, right_high) + dot(left_low, right_high) + dot(left_high, right_low)


CHUNKS = 4


def pack_kernel(flag_ref, real_hbm, imag_hbm, out_hbm, sums_hbm, packed, given, sums, arrive, leave, leave_sums):
    rows = BLOCK // CHUNKS
    sources = (real_hbm, imag_hbm)
    for c in range(CHUNKS):
        at = pl.ds(c * rows, rows)
        for part in range(2):
            pltpu.make_async_copy(sources[part].at[at], given.at[part, at], arrive.at[c]).start()
    squares = [jnp.zeros((SUB, LANES), f32) for _ in range(8)]
    diagonal = [jnp.zeros((SUB, LANES), f32) for _ in range(2)]
    for c in range(CHUNKS):
        both = given.at[:, pl.ds(c * rows, rows)]
        pltpu.make_async_copy(both, both, arrive.at[c]).wait()
        for h in range(c * rows // LOW, (c + 1) * rows // LOW):
            for t in range(BLOCK // LANES):
                for part in range(2):
                    quads = [
                        given[part, h * LOW + p * SUB : h * LOW + (p + 1) * SUB, t * LANES : (t + 1) * LANES]
                        for p in range(QUADS)
                    ]
                    for p, value in enumerate(quads):
                        squares[QUADS * part + p] += value * value
                    for q, value in enumerate(swap_quads(quads)):
                        slot = (h * GATE + t * QUADS + q) * SLOT
                        packed[slot + part * SUB : slot + (part + 1) * SUB, :] = value
        at = pl.ds(c * PAIRS * SLOT // CHUNKS, PAIRS * SLOT // CHUNKS)
        pltpu.make_async_copy(packed.at[at], out_hbm.at[at], leave).start()
        first = c * rows // LANES * LANES
        eye = iota((rows, LANES), 0) + (c * rows - first) == iota((rows, LANES), 1)
        for part in range(2):
            square = given[part, c * rows : (c + 1) * rows, first : first + LANES]
            kept = jnp.where(eye, square, jnp.zeros_like(square))
            diagonal[part] += jnp.sum(kept.reshape(rows // SUB, SUB, LANES), axis=0)

    def total(value):
        return jnp.sum(jnp.sum(value, axis=0, keepdims=True), axis=1, keepdims=True)

    lane = iota((1, LANES), 1)
    on_diagonal = flag_ref[0] == 1
    trace_real, trace_imag = (jnp.where(on_diagonal, total(value), 0.0) for value in diagonal)
    sums[...] = jnp.where(
        lane == 0,
        trace_real,
        jnp.where(lane == 1, trace_imag, jnp.where(lane == 2, total(sum(squares)), 0.0)),
    )
    leaving_sums = pltpu.make_async_copy(sums, sums_hbm, leave_sums)
    leaving_sums.start()
    pltpu.make_async_copy(packed, out_hbm, leave).wait()
    leaving_sums.wait()


def pack(flag, rho_real, rho_imag):
    return pl.pallas_call(
        pack_kernel,
        out_shape=[
            jax.ShapeDtypeStruct((PAIRS * SLOT, LANES), f32),
            jax.ShapeDtypeStruct((1, LANES), f32),
        ],
        in_specs=[SMEM, HBM, HBM],
        out_specs=[HBM, HBM],
        scratch_shapes=[
            pltpu.VMEM((PAIRS * SLOT, LANES), f32),
            pltpu.VMEM((2, BLOCK, BLOCK), f32),
            pltpu.VMEM((1, LANES), f32),
            pltpu.SemaphoreType.DMA((CHUNKS,)),
            pltpu.SemaphoreType.DMA,
            pltpu.SemaphoreType.DMA,
        ],
        compiler_params=pltpu.CompilerParams(vmem_limit_bytes=VMEM_ALL),
        name="pack",
    )(flag, rho_real, rho_imag)


def flip_rows(value, target):
    row = iota((LOW, LANES), 0)
    out = value
    for bit in range(LQ):
        step = 1 << bit
        up = pltpu.roll(value, LOW - step, 0)
        down = pltpu.roll(value, step, 0)
        flipped = jnp.where(jnp.bitwise_and(row, step) == 0, up, down)
        out = jnp.where(target == bit, flipped, out)
    return out


def factors_of(ref):
    return [
        tuple(ref.at[k * WIDE : (k + 1) * WIDE, half * WIDE : (half + 1) * WIDE] for half in range(2))
        for k in range(3)
    ]


def gates_kernel(angles_ref, targets_ref, order_ref, ur_ref, ui_ref, out_ref):
    row = iota((LOW, LANES), 0)
    lane = iota((LOW, LANES), 1)
    slot = iota((SUB, LANES), 0)
    half = jnp.zeros((SUB, LANES), f32)
    first = jnp.zeros((SUB, LANES), f32)
    second = jnp.zeros((SUB, LANES), f32)
    for k in range(GATES):
        gate = order_ref[k]
        half = jnp.where(slot == k, angles_ref[gate, 0], half)
        first = jnp.where(slot == k, angles_ref[gate, 1], first)
        second = jnp.where(slot == k, angles_ref[gate, 2], second)
    half = half / 2
    both = first + second
    c, s = jnp.cos(half), jnp.sin(half)
    entries = (
        (c, jnp.zeros_like(c)),
        (-jnp.cos(second) * s, -jnp.sin(second) * s),
        (jnp.cos(first) * s, jnp.sin(first) * s),
        (jnp.cos(both) * c, jnp.sin(both) * c),
    )
    unit = jnp.where(row == lane, 1.0, 0.0).astype(f32)
    products = [(unit, jnp.zeros_like(unit)), (unit, jnp.zeros_like(unit))]
    for k in range(GATES):
        target = targets_ref[order_ref[k]]
        high = jnp.bitwise_and(jnp.right_shift(row, target), 1) == 1
        low_low, low_high, high_low, high_high = (
            tuple(jnp.broadcast_to(member[k : k + 1, :], (LOW, LANES)) for member in entry)
            for entry in entries
        )
        same = [jnp.where(high, high_high[m], low_low[m]) for m in range(2)]
        other = [jnp.where(high, high_low[m], low_high[m]) for m in range(2)]
        for kind, (real, imag) in enumerate(products):
            flip_real = flip_rows(real, target)
            flip_imag = flip_rows(imag, target)
            new_real = same[0] * real - same[1] * imag + other[0] * flip_real - other[1] * flip_imag
            new_imag = same[0] * imag + same[1] * real + other[0] * flip_imag + other[1] * flip_real
            mine = (target < HIGH_LOW) == (kind == 0)
            products[kind] = (jnp.where(mine, new_real, real), jnp.where(mine, new_imag, imag))
    inner, outer = products

    def pick(size, index):
        return jnp.where(index(iota((LANES, size), 0)) == iota((LANES, size), 1), 1.0, 0.0).astype(f32)

    def expand(value, size, index):
        chosen = pick(size, index)

        def one(part):
            rows = jnp.dot(chosen, part, precision=highest, preferred_element_type=f32)
            return lax.dot_general(
                rows, chosen, (((1,), (1,)), ((), ())), precision=highest, preferred_element_type=f32
            )

        return tuple(one(part[:, :size]) for part in value)

    def times(left, right):
        return left[0] * right[0] - left[1] * right[1], left[0] * right[1] + left[1] * right[0]

    def conj(value):
        return value[0], -value[1]

    def transposed(value):
        return tuple(part[:, :LOW].T for part in value)

    flipped_inner, flipped_outer = transposed(inner), transposed(outer)
    group = expand(flipped_outer, LOW, lambda r: SUB * jnp.right_shift(r, LQ))
    own_high = expand(flipped_outer, LOW, lambda r: SUB * jnp.bitwise_and(jnp.right_shift(r, HIGH_LOW), QUADS - 1))
    own_sub = expand(flipped_inner, LOW, lambda r: jnp.bitwise_and(r, SUB - 1))
    right = times(group, conj(times(own_high, own_sub)))
    gate = (ur_ref[...], ui_ref[...])
    top = expand(gate, GATE, lambda r: jnp.right_shift(r, HIGH_LOW))
    sub = expand(inner, LOW, lambda r: jnp.bitwise_and(r, SUB - 1))
    rows_side = times(top, sub)
    same_sub = jnp.bitwise_and(iota((LANES, LANES), 0), SUB - 1) == jnp.bitwise_and(
        iota((LANES, LANES), 1), SUB - 1
    )
    cols_side = tuple(jnp.where(same_sub, KEEP * part, 0.0) for part in conj(top))

    refs = factors_of(out_ref)

    def place(which, at_row, at_col, value):
        for ref, part in zip(refs[which], split(value), strict=True):
            ref[at_row * LANES : (at_row + 1) * LANES, at_col * LANES : (at_col + 1) * LANES] = part

    for which, (real, imag), sign in ((0, right, -1), (1, rows_side, 1), (2, cols_side, 1)):
        place(which, 0, 0, real)
        place(which, 0, 1, -sign * imag)
        place(which, 1, 0, sign * imag)
        place(which, 1, 1, real)


def gates(angles, targets, gate_order, gate_real, gate_imag):
    return pl.pallas_call(
        gates_kernel,
        out_shape=jax.ShapeDtypeStruct((3 * WIDE, 2 * WIDE), bf16),
        in_specs=[SMEM, SMEM, SMEM, VMEM, VMEM],
        out_specs=VMEM,
        compiler_params=pltpu.CompilerParams(vmem_limit_bytes=VMEM_LIMIT),
        cost_estimate=pl.CostEstimate(flops=40_000_000, bytes_accessed=800_000, transcendentals=8192),
        name="gates",
    )(angles, targets, gate_order, gate_real, gate_imag)


def apply_kernel(
    flag_ref, sums_ref, got, factors, real_hbm, imag_hbm, purity_hbm,
    first_done, second_done, real, imag, purity, leave, leave_purity,
):
    right, rows_side, cols_side = ([half[...] for half in pair] for pair in factors_of(factors))
    for g in range(GATE):
        slots = got[g * GATE * SLOT : (g + 1) * GATE * SLOT, :].reshape(GATE, SLOT, LANES)
        value = jnp.concatenate(
            [slots[:, part * SUB : (part + 1) * SUB, :].reshape(LANES, LANES) for part in range(2)], axis=1
        )
        value = three_pass(split(value), right)
        for part in range(2):
            first_done[part, g] = value[:, part * LANES : (part + 1) * LANES].reshape(GATE, SUB, LANES)

    for g in range(0, GATE, 2):
        value = jnp.concatenate(
            [
                jnp.concatenate([first_done[part, :, g + k].reshape(LANES, LANES) for part in range(2)], axis=0)
                for k in range(2)
            ],
            axis=1,
        )
        value = three_pass(rows_side, split(value))
        for k in range(2):
            for part in range(2):
                second_done[part, :, g + k] = value[
                    part * LANES : (part + 1) * LANES, k * LANES : (k + 1) * LANES
                ].reshape(GATE, SUB, LANES)

    sums = sums_ref[...]
    lane = iota((1, LANES), 1)
    trace_real, trace_imag, squares = (jnp.sum(jnp.where(lane == k, sums, 0.0)) for k in range(3))
    purity[0, 0] = (
        KEEP * KEEP * squares
        + (2 * KEEP * MIXING + MIXING * MIXING) * (trace_real * trace_real + trace_imag * trace_imag) / DIM
    ) / (DIM * DIM)
    leaving_purity = pltpu.make_async_copy(purity, purity_hbm, leave_purity)
    leaving_purity.start()
    shifts = [
        jnp.where(flag_ref[0] == 1, MIXING * trace / DIM, 0.0) for trace in (trace_real, trace_imag)
    ]

    for g in range(0, GATE, 2):
        value = jnp.concatenate(
            [
                jnp.concatenate([second_done[part, g + k].reshape(LANES, LANES) for part in range(2)], axis=0)
                for k in range(2)
            ],
            axis=1,
        )
        value = three_pass(cols_side, split(value))
        for k in range(2):
            for part, ref in enumerate((real, imag)):
                block = value[part * LANES : (part + 1) * LANES, k * LANES : (k + 1) * LANES]
                for t in range(GATE // QUADS):
                    quads = swap_quads(
                        [block[(t * QUADS + q) * SUB : (t * QUADS + q + 1) * SUB, :] for q in range(QUADS)]
                    )
                    for p in range(QUADS):
                        at = (g + k) * LOW + p * SUB
                        out = quads[p]
                        if t == (g + k) // QUADS:
                            eye = iota((SUB, LANES), 0) + ((g + k) % QUADS * LOW + p * SUB) == iota((SUB, LANES), 1)
                            out = out + jnp.where(eye, shifts[part], 0.0)
                        ref[at : at + SUB, t * LANES : (t + 1) * LANES] = out
        at = pl.ds(g * LOW, 2 * LOW)
        for part, ref in enumerate((real, imag)):
            pltpu.make_async_copy(ref.at[at], (real_hbm, imag_hbm)[part].at[at], leave.at[part]).start(priority=part)
    for part, ref in enumerate((real, imag)):
        pltpu.make_async_copy(ref, (real_hbm, imag_hbm)[part], leave.at[part]).wait()
    leaving_purity.wait()


def apply(flag, sums, got, factors):
    return pl.pallas_call(
        apply_kernel,
        out_shape=[
            jax.ShapeDtypeStruct((BLOCK, BLOCK), f32),
            jax.ShapeDtypeStruct((BLOCK, BLOCK), f32),
            jax.ShapeDtypeStruct((1, 1), f32),
        ],
        in_specs=[SMEM, VMEM, VMEM, VMEM],
        out_specs=[HBM, HBM, HBM],
        scratch_shapes=[
            pltpu.VMEM((2, GATE, GATE, SUB, LANES), f32),
            pltpu.VMEM((2, GATE, GATE, SUB, LANES), f32),
            pltpu.VMEM((BLOCK, BLOCK), f32),
            pltpu.VMEM((BLOCK, BLOCK), f32),
            pltpu.SMEM((1, 1), f32),
            pltpu.SemaphoreType.DMA((2,)),
            pltpu.SemaphoreType.DMA,
        ],
        compiler_params=pltpu.CompilerParams(vmem_limit_bytes=VMEM_LIMIT),
        name="apply",
    )(flag, sums, got, factors)


def sum_everywhere(value):
    for axis in ROW_COL:
        if axis != RING:
            value = lax.psum(value, axis)
    size = lax.axis_size(RING)
    shifted = [
        lax.ppermute(value, RING, [(i, (i + k) % size) for i in range(size)]) for k in range(1, size)
    ]
    return value + sum(shifted)


def on_device(rho_real, rho_imag, gate_real, gate_imag, angles, targets, gate_order):
    flag = (lax.axis_index(ROW) == lax.axis_index(COL)).astype(jnp.int32).reshape(1)
    sent, sums = pack(flag, rho_real, rho_imag)
    got = lax.all_to_all(
        sent.reshape(PAIRS, 1, SLOT * LANES), ROW_COL, split_axis=0, concat_axis=0, tiled=True
    ).reshape(PAIRS * SLOT, LANES)
    sums = sum_everywhere(sums)
    factors = gates(angles, targets, gate_order, gate_real, gate_imag)
    mixed_real, quadrature, purity = apply(flag, sums, got, factors)
    return mixed_real, quadrature, purity.reshape(())


def solution(mesh):
    split_mesh = Mesh(mesh.devices.reshape(2, 4, 2, 8, 2), ROW_COL)
    placed = (P(ROW, COL), P(ROW, COL), P(), P(), P(), P(), P())
    return jax.shard_map(
        on_device,
        mesh=split_mesh,
        in_specs=placed,
        out_specs=(P(ROW, COL), P(ROW, COL), P()),
        check_vma=False,
    )
```
